512 devices in a mesh: angle: 2 (over y), row: 128 (over z, x), col: 2 (over core).
Axes of the slice: x: 4, y: 2, z: 32, core: 2. Of those that a mesh axis runs over, the one named last changes fastest.
The devices are a block of a 4x8x32 slice.
Arguments:
- obj_field: float32 [2, 32768, 1024], P(None, ('angle', 'row'), 'col'), parts along dimension 1, may hold values from -6 to 6
- probe_modes: bfloat16 [2, 6, 256, 256], replicated, may hold values from -6 to 6
- centers: int32 [512, 2], P(('angle', 'row', 'col')), parts along dimension 0, may hold values from 0 to 16383, as said below
- amplitudes: float32 [512, 256, 256], P(('angle', 'row', 'col')), parts along dimension 0, may hold values from 0.2 to 4
Outputs:
- new_object: float32 [2, 32768, 1024], P(None, ('angle', 'row'), 'col'), parts along dimension 1
- new_probe: float32 [2, 12, 256, 256], P(None, 'angle'), parts along dimension 1
The draws below stay inside these ranges and needn't reach their ends.
There are 2 independent parts, one for each index of `angle`. The reference program is written for one: setup_inputs(seed, part) draws one part's arguments, and reference() takes and returns one part's arrays. A program takes and returns all parts, laid end to end along the dimension named above; an argument that names none is the same for every part. Nothing has to cross between parts.
Inputs may be any that keep to these rules, and one draw needn't show every extreme that they name: `centers`: position k belongs to device d = k // 1 of the row+col order (row slowest); its centre lies in that device's tile: row in [(d // (1024 // 512)) * 128, + 128), column in [(d % (1024 // 512)) * 512, + 512).
All inputs are finite; a program needn't handle non-finite values.
Results may differ from the reference program's by a relative error of at most 0.0003.
Values sent between devices are 32-bit elements; how exact they have to be, the bound alone decides.
A program may use at most 64 MiB of HBM per device.

```python
import math
import jax
import jax.numpy as jnp
from jax import lax

P_SIZE = 256
MODES = 6
TILE_R = 128
TILE_C = 512
POS_DEV = 1
OBJ_ROWS = 16384
OBJ_COLS = 1024
POSITIONS = 256


def draw_centers(key, part):
    first_key, second_key = jax.random.split(jax.random.fold_in(key, 11))
    owner = jnp.arange(POSITIONS, dtype=jnp.int32) // POS_DEV
    tiles_across = OBJ_COLS // TILE_C
    tile_row = owner // tiles_across
    tile_col = owner % tiles_across
    rows_drawn = tile_row * TILE_R + jax.random.randint(first_key, (POSITIONS,), 0, TILE_R)
    cols_drawn = tile_col * TILE_C + jax.random.randint(second_key, (POSITIONS,), 0, TILE_C)
    return jnp.stack([rows_drawn, cols_drawn], axis=1).astype(jnp.int32)


def steps_of(key, extent, cuts, smallest, largest):
    def one(axis_at, shards_of):
        steps = jax.random.uniform(jax.random.fold_in(jax.random.fold_in(key, 6), axis_at), (shards_of,), jnp.float32, smallest / len(cuts), largest / len(cuts))
        return jnp.repeat(jnp.exp(steps), extent[axis_at] // shards_of).reshape((-1,) + (1,) * (len(extent) - axis_at - 1))

    gain = one(*cuts[0])
    for cut in cuts[1:]:
        gain = gain * one(*cut)
    return gain


def scatter_about(own_key, extent, width, most, shards=(), kind=jnp.bfloat16):
    gain = steps_of(own_key, extent, shards, -0.22, 0.18) if shards else 1.0
    entries = jax.random.normal(own_key, extent, jnp.float32) * width * gain
    return jnp.minimum(jnp.maximum(entries, -most), most).astype(kind)


def setup_inputs(seed: int = 0, part: int = 0) -> dict:
    splits = jax.random.split(jax.random.key(seed), 5)
    own_keys = jax.random.split(jax.random.fold_in(splits[4], part), 5)
    return {
        "obj_field": scatter_about(own_keys[0], (2, OBJ_ROWS, OBJ_COLS), 1.0, 6.0, ((1, 128), (2, 2)), jnp.float32),
        "probe_modes": scatter_about(splits[1], (2, MODES, P_SIZE, P_SIZE), 1.0, 6.0),
        "centers": draw_centers(jax.random.fold_in(jax.random.fold_in(splits[4], part), 71), part),
        "amplitudes": jnp.clip(jnp.exp(math.log(4.0) - 2.9957323 * jax.random.uniform(own_keys[3], (POSITIONS, P_SIZE, P_SIZE), jnp.float32) ** steps_of(own_keys[3], (POSITIONS, P_SIZE, P_SIZE), ((0, 256),), -0.2, 0.2)), 0.2, 4.0),
    }


def reference(obj_field, probe_modes, centers, amplitudes):
    margin = P_SIZE // 2
    probe = probe_modes.astype(jnp.float32)
    probe_real = probe[0]
    probe_imag = probe[1]
    spot_map = lax.optimization_barrier(jnp.sum(probe_real * probe_real + probe_imag * probe_imag, axis=0))
    padded = jnp.pad(obj_field, ((0, 0), (margin, margin), (margin, margin)))
    anchor = jnp.zeros((), jnp.int32)

    def visit_position(totals, inputs):
        buffer, probe_grad, probe_weight = totals
        center, measured = inputs
        row_start = center[0].astype(jnp.int32)
        col_start = center[1].astype(jnp.int32)
        window = lax.dynamic_slice(padded, (anchor, row_start, col_start), (2, P_SIZE, P_SIZE))
        win_real = window[0]
        win_imag = window[1]
        exit_real = probe_real * win_real - probe_imag * win_imag
        exit_imag = probe_real * win_imag + probe_imag * win_real
        far_field = jnp.fft.fft2(lax.complex(exit_real, exit_imag), norm='ortho')
        far_real = jnp.real(far_field)
        far_imag = jnp.imag(far_field)
        modulus = jnp.sqrt(lax.optimization_barrier(jnp.sum(far_real * far_real + far_imag * far_imag, axis=0)))
        factor = measured / (modulus + 0.5)
        back_wave = jnp.fft.ifft2(lax.complex(far_real * factor, far_imag * factor), norm='ortho')
        diff_real = jnp.real(back_wave) - exit_real
        diff_imag = jnp.imag(back_wave) - exit_imag
        obj_real = lax.optimization_barrier(jnp.sum(probe_real * diff_real + probe_imag * diff_imag, axis=0))
        obj_imag = lax.optimization_barrier(jnp.sum(probe_real * diff_imag - probe_imag * diff_real, axis=0))
        stacked = jnp.stack([obj_real, obj_imag, spot_map])
        current = lax.dynamic_slice(buffer, (anchor, row_start, col_start), (3, P_SIZE, P_SIZE))
        buffer = lax.dynamic_update_slice(buffer, current + stacked, (anchor, row_start, col_start))
        probe_grad = probe_grad + jnp.stack([win_real * diff_real + win_imag * diff_imag, win_real * diff_imag - win_imag * diff_real])
        probe_weight = probe_weight + win_real * win_real + win_imag * win_imag
        return ((buffer, probe_grad, probe_weight), None)
    start_state = (jnp.zeros((3, OBJ_ROWS + 2 * margin, OBJ_COLS + 2 * margin), jnp.float32), jnp.zeros((2, MODES, P_SIZE, P_SIZE), jnp.float32), jnp.zeros((P_SIZE, P_SIZE), jnp.float32))
    final_state, unused = lax.scan(visit_position, start_state, (centers, amplitudes))
    buffer, probe_grad, probe_weight = final_state
    interior = buffer[:, margin:margin + OBJ_ROWS, margin:margin + OBJ_COLS]
    illumination = interior[2]
    peak_value = jnp.max(illumination)
    new_object = obj_field + interior[:2] / (illumination + 0.1 * peak_value)
    peak_weight = jnp.max(probe_weight)
    new_probe = probe + probe_grad / (probe_weight + 0.1 * peak_weight)
    return (new_object, new_probe)
```

```python
import functools
import math

import jax
import jax.numpy as jnp
import numpy as np
from jax import lax
from jax.experimental import pallas as pl
from jax.experimental.pallas import tpu as pltpu
from jax.sharding import Mesh
from jax.sharding import PartitionSpec as P

ROW = ("row_0", "row_1")
ANGLE_ROW = ("angle", "row_0", "row_1")
ANGLE_ROW_COL = ("angle", "row_0", "row_1", "col")
VMEM_LIMIT = 60 * 1024 * 1024
ORDER = ((0, 1, 2, 3), False, (0, 3, 5))
MESHID = pl.DeviceIdType.MESH
LANES = 128
NEAR = 4


class Exchange:
    def __init__(self, send_sems, recv_sems, first):
        self.send_sems, self.recv_sems, self.next = send_sems, recv_sems, first
        self.copies = []

    def send(self, src, dst, peer):
        copy = pltpu.make_async_remote_copy(
            src_ref=src,
            dst_ref=dst,
            send_sem=self.send_sems.at[self.next],
            recv_sem=self.recv_sems.at[self.next],
            device_id=peer,
            device_id_type=MESHID,
        )
        copy.start()
        self.next += 1
        self.copies.append(copy)


def rows_at(ref, start, size):
    return ref.at[pl.ds(pl.multiple_of(start, 8), size), :]


def far_order(count):
    return sorted(range(1, count), key=lambda d: -min(d, count - d))


COPIES_PER_CHUNK = 64


def all_sum_kernel(chunks, far, order, x_ref, m_ref, upd_ref, o_ref, om_ref, pair_ref, part_ref, *scratch):
    scratch = list(scratch)
    send_sems, recv_sems = scratch[-2:]
    c, x, z = lax.axis_index("col"), lax.axis_index("row_1"), lax.axis_index("row_0")
    near_at, far_at = lax.rem(z, NEAR), lax.div(z, NEAR)
    partner = {"col": 1 - c}
    x_one = {"row_1": x + 1 - 2 * lax.rem(x, 2)}
    x_two = {"row_1": 3 - x}
    near_peers = {d: {"row_0": far_at * NEAR + lax.rem(near_at + d, NEAR)} for d in range(1, NEAR)}
    far_peers = {d: {"row_0": lax.rem(far_at + d, far) * NEAR + near_at} for d in range(1, far)}
    near_order, far_list = far_order(NEAR), far_order(far)
    barrier = pltpu.get_barrier_semaphore()
    up, down = row_neighbours(x, z, 4, far * NEAR)
    peers = [partner, x_one, x_two, up, down, *near_peers.values(), *far_peers.values()]
    for peer in peers:
        pl.semaphore_signal(barrier, inc=1, device_id=peer, device_id_type=MESHID)
    pl.semaphore_wait(barrier, len(peers))

    mine, theirs = (
        pl.ds(pl.multiple_of(c * LANES, LANES), LANES),
        pl.ds(pl.multiple_of((1 - c) * LANES, LANES), LANES),
    )
    bit_a = lax.rem(lax.div(x + 1, 2), 2)
    bit_b = lax.div(x, 2)
    keep_one, peer_one = (bit_a, bit_b), (x_one, x_two)
    keep_two, peer_two = (bit_b, bit_a), (x_two, x_one)

    class Chunk:
        def __init__(self, index, start, rows, bufs):
            self.start, self.rows, self.bufs = start, rows, bufs
            self.next = index * COPIES_PER_CHUNK
            self.spread = rows // 128 >= 8
            self.pending = None

        def exchange(self):
            self.pending = Exchange(send_sems, recv_sems, self.next)
            return self.pending

        def arrive(self):
            for copy in self.pending.copies:
                copy.wait()
            self.next = self.pending.next

        def step(self, s):
            R, b = self.rows, self.bufs
            if s > 0:
                self.arrive()
            if s == 0:
                e = self.exchange()
                e.send(x_ref.at[pl.ds(self.start, R), theirs], b["rc"], partner)
            elif s == 1:
                b["s0"][...] = x_ref[pl.ds(self.start, R), mine] + b["rc"][...]
                e = self.exchange()
                for h in range(2):
                    src = rows_at(b["s0"], h * (R // 2) + (1 - keep_one[h]) * (R // 4), R // 4)
                    e.send(src, b["r1"].at[h], peer_one[h])
            elif s == 2:
                for h in range(2):
                    kept = pl.ds(pl.multiple_of(h * (R // 2) + keep_one[h] * (R // 4), 8), R // 4)
                    b["s1"][h] = b["s0"][kept, :] + b["r1"][h]
                e = self.exchange()
                for h in range(2):
                    src = rows_at(b["s1"].at[h], (1 - keep_two[h]) * (R // 8), R // 8)
                    e.send(src, b["r2"].at[h], peer_two[h])
            elif s == 3:
                for h in range(2):
                    kept = pl.ds(pl.multiple_of(keep_two[h] * (R // 8), 8), R // 8)
                    b["s2"][pl.ds(h * (R // 8), R // 8), :] = b["s1"][h, kept, :] + b["r2"][h]
                e = self.exchange()
                for d in near_order:
                    src = rows_at(b["s2"], lax.rem(near_at + d, NEAR) * (R // 16), R // 16)
                    e.send(src, b["r3"].at[d - 1], near_peers[d])
            elif s == 4:
                kept = pl.ds(pl.multiple_of(near_at * (R // 16), 8), R // 16)
                total = b["s2"][kept, :]
                for d in range(1, NEAR):
                    total = total + b["r3"][d - 1]
                b["s3"][...] = total
                e = self.exchange()
                for d in far_list:
                    if self.spread:
                        src = rows_at(b["s3"], lax.rem(far_at + d, far) * (R // 128), R // 128)
                    else:
                        src = b["s3"]
                    e.send(src, b["r4"].at[d - 1], far_peers[d])
            elif s == 5:
                if self.spread:
                    at = pl.ds(pl.multiple_of(far_at * (R // 128), 8), R // 128)
                    total = b["s3"][at, :]
                    for d in range(1, far):
                        total = total + b["r4"][d - 1]
                    b["g3"][at, :] = total
                    e = self.exchange()
                    block = rows_at(b["g3"], far_at * (R // 128), R // 128)
                    for d in far_list:
                        e.send(block, block, far_peers[d])
                else:
                    b["r4"][far - 1] = b["s3"][...]
                    total = jnp.zeros((R // 16, LANES), jnp.float32)
                    for owner in range(far):
                        total = total + b["r4"][lax.rem(far_at - owner + far - 1, far)]
                    b["g3"][...] = total
                    self.exchange()
            elif s == 6:
                at = pl.ds(pl.multiple_of(near_at * (R // 16), 8), R // 16)
                e = self.exchange()
                dst = rows_at(b["g2"], near_at * (R // 16), R // 16)
                for d in near_order:
                    e.send(b["g3"], dst, near_peers[d])
                b["g2"][at, :] = b["g3"][...]
            elif s == 7:
                e = self.exchange()
                for h in range(2):
                    src = rows_at(b["g2"], h * (R // 8), R // 8)
                    dst = rows_at(b["g1"].at[h], keep_two[h] * (R // 8), R // 8)
                    e.send(src, dst, peer_two[h])
                for h in range(2):
                    at = pl.ds(pl.multiple_of(keep_two[h] * (R // 8), 8), R // 8)
                    b["g1"][h, at, :] = b["g2"][pl.ds(h * (R // 8), R // 8), :]
            elif s == 8:
                e = self.exchange()
                for h in range(2):
                    dst = rows_at(b["g0"], h * (R // 2) + keep_one[h] * (R // 4), R // 4)
                    e.send(b["g1"].at[h], dst, peer_one[h])
                for h in range(2):
                    at = pl.ds(pl.multiple_of(h * (R // 2) + keep_one[h] * (R // 4), 8), R // 4)
                    b["g0"][at, :] = b["g1"][h]
            elif s == 9:
                e = self.exchange()
                e.send(b["g0"], o_ref.at[pl.ds(self.start, R), mine], partner)
                o_ref[pl.ds(self.start, R), mine] = b["g0"][...]

    class Peak:
        def __init__(self, index, bufs):
            self.next, self.bufs = index * COPIES_PER_CHUNK, bufs
            self.stages = [[partner], [x_one], [x_two], list(near_peers.values()), list(far_peers.values())]
            self.slot = 0
            self.copies = []

        def step(self, s):
            held, came = self.bufs["held"], self.bufs["came"]
            if s > 0:
                top = m_ref[...] if s == 1 else held[s - 1]
                for i, copy in enumerate(self.copies):
                    copy.wait()
                    top = jnp.maximum(top, came[self.slot - len(self.copies) + i])
                if s == 5:
                    om_ref[...] = top
                    return
                held[s] = top
            e = Exchange(send_sems, recv_sems, self.next)
            for peer in self.stages[s]:
                e.send(m_ref if s == 0 else held.at[s], came.at[self.slot], peer)
                self.slot += 1
            self.next, self.copies = e.next, e.copies

    class Fold:
        def __init__(self, index):
            self.index = index

        def step(self, s):
            half = upd_ref.shape[1] // 2
            if s == 0:
                self.first = Exchange(send_sems, recv_sems, self.index * COPIES_PER_CHUNK)
                self.first.send(upd_ref.at[:, pl.ds(half, half), :], part_ref.at[0, c], down)
                self.first.send(upd_ref.at[:, pl.ds(0, half), :], part_ref.at[1, c], up)
                self.first.send(upd_ref, pair_ref, partner)
            elif s == 1:
                self.last = Exchange(send_sems, recv_sems, self.index * COPIES_PER_CHUNK + 8)
                for i in range(2):
                    self.first.copies[i].wait()
                    self.last.send(part_ref.at[i, c], part_ref.at[i, c], partner)
                self.first.copies[2].wait()
            else:
                for copy in self.last.copies:
                    copy.wait()

    fold = Fold(len(chunks) + 1)
    objects = []
    at = 0
    for i, (start, rows) in enumerate(chunks):
        names = chunk_buffers(rows, far)
        bufs = dict(zip(names, scratch[at : at + len(names)]))
        at += len(names)
        objects.append(Chunk(i, start, rows, bufs))
    peak = Peak(len(chunks), dict(held=scratch[at], came=scratch[at + 1]))
    for which, s in order:
        if which == -1:
            peak.step(s)
        elif which == -2:
            fold.step(s)
        else:
            objects[which].step(s)
    for o in objects:
        o.arrive()


def chunk_buffers(rows, far):
    R = rows
    last = R // 128 if R // 128 >= 8 else R // 16
    return dict(
        rc=(R, LANES), s0=(R, LANES), r1=(2, R // 4, LANES), s1=(2, R // 4, LANES), r2=(2, R // 8, LANES),
        s2=(R // 4, LANES), r3=(NEAR - 1, R // 16, LANES), s3=(R // 16, LANES), r4=(far, last, LANES),
        g3=(R // 16, LANES), g2=(R // 4, LANES), g1=(2, R // 4, LANES), g0=(R, LANES),
    )


def wave(count, lags, early, fold_at):
    order = []
    for t in range(10 + max(lags)):
        if t in fold_at:
            order.append((-2, fold_at.index(t)))
        ready = [(i, t - lags[i]) for i in range(count) if 0 <= t - lags[i] < 10]
        order += ready if early else ready[::-1]
        if t < 6:
            order.append((-1, t))
    return order


def all_sum(x, m, upd, far, chunks, order):
    bufs = []
    for _, rows in chunks:
        bufs += [pltpu.VMEM(s, jnp.float32) for s in chunk_buffers(rows, far).values()]
    bufs += [pltpu.VMEM((6, 8, LANES), jnp.float32), pltpu.VMEM((3 + NEAR - 1 + far - 1, 8, LANES), jnp.float32)]
    count = COPIES_PER_CHUNK * (len(chunks) + 2)
    side = upd.shape[1]
    shapes = (x.shape, m.shape, upd.shape, (2, 2, 2, side // 2, side))
    return pl.pallas_call(
        functools.partial(all_sum_kernel, chunks, far, order),
        out_shape=tuple(jax.ShapeDtypeStruct(shape, jnp.float32) for shape in shapes),
        in_specs=[pl.BlockSpec(memory_space=pltpu.VMEM)] * 3,
        out_specs=(pl.BlockSpec(memory_space=pltpu.VMEM),) * 4,
        scratch_shapes=bufs + [pltpu.SemaphoreType.DMA((count,)), pltpu.SemaphoreType.DMA((count,))],
        compiler_params=pltpu.CompilerParams(collective_id=0, has_side_effects=True, vmem_limit_bytes=VMEM_LIMIT),
        name="all_sum",
    )(x, m, upd)


def dft_tables(side):
    half = side // 2
    n, q = np.arange(half)[None, :], np.arange(half)[:, None]
    tables = []
    for odd in range(2):
        phase = 2.0 * np.pi * ((n * (2 * q + odd)) % side) / side
        cosine, sine = np.cos(phase) / math.sqrt(side), np.sin(phase) / math.sqrt(side)
        table = np.block([[cosine, sine], [-sine, cosine]])
        tables += [table, table.T]
    tables = np.stack(tables).astype(np.float32)
    high = tables.astype(jnp.bfloat16)
    low = (tables - high.astype(np.float32)).astype(jnp.bfloat16)
    return np.stack([high, low], axis=1)


def order_table(side):
    table = np.zeros((side, side), np.float32)
    at = np.arange(side)
    table[at, np.where(at < side // 2, 2 * at, 2 * at + 1 - side)] = 1.0
    return table.astype(jnp.bfloat16)


def halves(value):
    high = value.astype(jnp.bfloat16)
    return high, (value - high.astype(jnp.float32)).astype(jnp.bfloat16)


def dot(a, b):
    return jnp.dot(a, b, preferred_element_type=jnp.float32)


def from_left(tab_ref, which, value):
    high, low = halves(value)
    return dot(tab_ref[which, 0], high) + dot(tab_ref[which, 0], low) + dot(tab_ref[which, 1], high)


def from_right(tab_ref, which, value):
    high, low = halves(value)
    return dot(high, tab_ref[which, 0]) + dot(low, tab_ref[which, 0]) + dot(high, tab_ref[which, 1])


def to_far_field(tab_ref, re, im):
    h = re.shape[0] // 2
    plus = jnp.concatenate([re[:h] + re[h:], im[:h] + im[h:]], axis=0)
    minus = jnp.concatenate([re[:h] - re[h:], im[:h] - im[h:]], axis=0)
    even, odd = from_left(tab_ref, 0, plus), from_left(tab_ref, 2, minus)
    re = jnp.concatenate([even[:h], odd[:h]], axis=0)
    im = jnp.concatenate([even[h:], odd[h:]], axis=0)
    plus = jnp.concatenate([re[:, :h] + re[:, h:], im[:, :h] + im[:, h:]], axis=1)
    minus = jnp.concatenate([re[:, :h] - re[:, h:], im[:, :h] - im[:, h:]], axis=1)
    even, odd = from_right(tab_ref, 1, plus), from_right(tab_ref, 3, minus)
    re = jnp.concatenate([even[:, :h], odd[:, :h]], axis=1)
    im = jnp.concatenate([even[:, h:], odd[:, h:]], axis=1)
    return re, im


def from_far_field(tab_ref, re, im):
    h = re.shape[0] // 2
    even = from_right(tab_ref, 0, jnp.concatenate([re[:, :h], im[:, :h]], axis=1))
    odd = from_right(tab_ref, 2, jnp.concatenate([re[:, h:], im[:, h:]], axis=1))
    plus, minus = even + odd, even - odd
    re = jnp.concatenate([plus[:, :h], minus[:, :h]], axis=1)
    im = jnp.concatenate([plus[:, h:], minus[:, h:]], axis=1)
    even = from_left(tab_ref, 1, jnp.concatenate([re[:h], im[:h]], axis=0))
    odd = from_left(tab_ref, 3, jnp.concatenate([re[h:], im[h:]], axis=0))
    plus, minus = even + odd, even - odd
    re = jnp.concatenate([plus[:h], minus[:h]], axis=0)
    im = jnp.concatenate([plus[h:], minus[h:]], axis=0)
    return re, im


def reorder(order_ref, value):
    def three(v):
        high, rest = v.astype(jnp.bfloat16), None
        rest = v - high.astype(jnp.float32)
        middle = rest.astype(jnp.bfloat16)
        return high, middle, (rest - middle.astype(jnp.float32)).astype(jnp.bfloat16)

    table = order_ref[...]
    high, middle, low = three(value)
    value = dot(table, high) + dot(table, middle) + dot(table, low)
    across = lambda v: lax.dot_general(
        v, table, (((1,), (1,)), ((), ())), preferred_element_type=jnp.float32
    )
    high, middle, low = three(value)
    return across(high) + across(middle) + across(low)


def from_row(ref, row, rows, cols):
    off = lax.rem(row, 8)
    value = ref[pl.ds(pl.multiple_of(row - off, 8), rows + 8), cols]
    return pltpu.roll(value, lax.rem(rows + 8 - off, rows + 8), 0)[:rows]


def add_window(acc_ref, source_ref, row, col, scale=None):
    rows = acc_ref.shape[0]
    side = source_ref.shape[1]
    value = from_row(source_ref, row, rows, slice(None))
    if scale is not None:
        value = jnp.where(scale > 0, value, 0.0)
    value = jnp.concatenate([value, jnp.zeros((rows, LANES), jnp.float32)], axis=1)
    value = pltpu.roll(value, lax.rem(col, LANES), 1)
    at = pl.ds(pl.multiple_of(lax.div(col, LANES) * LANES, LANES), side + LANES)
    acc_ref[:, at] = acc_ref[:, at] + value


def sources(cent_ref, tile_cols, margin):
    c = cent_ref[6, 0]
    for where in range(3):
        for side_col in range(2):
            k = where * 2 + side_col
            row = margin - cent_ref[k, 0]
            col = (side_col - c) * tile_cols + cent_ref[k, 1] - margin + tile_cols + margin
            there = jnp.int32(1)
            if where == 0:
                there = cent_ref[7, 0]
            if where == 2:
                there = cent_ref[7, 1]
            yield where, side_col, row, col, there


def wave_kernel(
    cent_ref, ext_ref, probe_ref, amp_ref, tab_ref, order_ref,
    sum_ref, upd_ref, illum_ref, top_ref,
    win, far, amp, acc, shifted,
):
    modes, side = probe_ref.shape[1], probe_ref.shape[2]
    margin = side // 2
    tile_rows, tile_cols = illum_ref.shape
    c = cent_ref[6, 0]
    own_row, own_col = cent_ref[2 + c, 0], cent_ref[2 + c, 1]
    shift = lax.rem(own_col, LANES)
    at = pl.ds(pl.multiple_of(own_col - shift, LANES), side + LANES)
    for p in range(2):
        value = from_row(ext_ref.at[p], own_row, side, at)
        value = pltpu.roll(value, lax.rem(side + LANES - shift, side + LANES), 1)
        win[p] = value[:, :side]
    sum_ref[pl.ds(2 * modes * side, side), :] = win[0] * win[0] + win[1] * win[1]
    shifted[pl.ds(0, side), :] = jnp.zeros((side, side), jnp.float32)
    amp[...] = jnp.zeros_like(amp)

    def forward(m, carry):
        pr, pi = probe_ref[0, m].astype(jnp.float32), probe_ref[1, m].astype(jnp.float32)
        re, im = to_far_field(tab_ref, pr * win[0] - pi * win[1], pr * win[1] + pi * win[0])
        far[m, 0], far[m, 1] = re, im
        amp[...] += re * re + im * im
        shifted[pl.ds(0, side), :] += pr * pr + pi * pi
        return carry

    lax.fori_loop(0, modes, forward, 0)
    amp[...] = reorder(order_ref, amp_ref[0]) / (jnp.sqrt(amp[...]) + 0.5)
    upd_ref[...] = jnp.zeros_like(upd_ref)

    def backward(m, carry):
        factor = amp[...]
        re, im = from_far_field(tab_ref, far[m, 0] * factor, far[m, 1] * factor)
        pr, pi = probe_ref[0, m].astype(jnp.float32), probe_ref[1, m].astype(jnp.float32)
        wr, wi = win[0], win[1]
        re = re - (pr * wr - pi * wi)
        im = im - (pr * wi + pi * wr)
        upd_ref[0] += pr * re + pi * im
        upd_ref[1] += pr * im - pi * re
        at_re, at_im = pl.multiple_of(m * side, 8), pl.multiple_of((modes + m) * side, 8)
        sum_ref[pl.ds(at_re, side), :] = wr * re + wi * im
        sum_ref[pl.ds(at_im, side), :] = wr * im - wi * re
        return carry

    lax.fori_loop(0, modes, backward, 0)

    zeros = jnp.zeros((margin, side), jnp.float32)
    spot_top, spot_bottom = shifted[pl.ds(0, margin), :], shifted[pl.ds(margin, margin), :]
    acc[...] = jnp.zeros_like(acc)
    laid = {0: (spot_bottom, zeros), 1: (spot_top, spot_bottom), 2: (zeros, spot_top)}
    for where, side_col, row, col, there in sources(cent_ref, tile_cols, margin):
        if side_col == 0:
            shifted[pl.ds(0, margin), :], shifted[pl.ds(margin, margin), :] = laid[where]
        add_window(acc, shifted, row, col, there)
    total = acc[:, pl.ds(tile_cols + margin, tile_cols)]
    illum_ref[...] = total
    top_ref[...] = jnp.full(top_ref.shape, jnp.max(total))


def place_kernel(
    cent_ref, obj_ref, probe_ref, upd_ref, pair_ref, part_ref, illum_ref, top_ref, sum_ref,
    new_obj_ref, new_probe_ref, acc, shifted,
):
    modes, side = probe_ref.shape[1], probe_ref.shape[2]
    margin = side // 2
    tile_cols = illum_ref.shape[1]
    c = cent_ref[6, 0]
    below = illum_ref[...] + 0.1 * jnp.max(top_ref[...])
    for p in range(2):
        acc[...] = jnp.zeros_like(acc)
        for where, side_col, row, col, there in sources(cent_ref, tile_cols, margin):
            if where == 1:
                shifted[pl.ds(0, side), :] = jnp.where(c == side_col, upd_ref[p], pair_ref[p])
            else:
                part = part_ref[where // 2, side_col, p]
                first = where // 2 * margin
                shifted[pl.ds(first, margin), :] = part
                shifted[pl.ds(margin - first, margin), :] = jnp.zeros((margin, side), jnp.float32)
            add_window(acc, shifted, row, col, there)
        new_obj_ref[p] = obj_ref[p] + acc[:, pl.ds(tile_cols + margin, tile_cols)] / below
    weight = sum_ref[pl.ds(2 * modes * side, side), :]
    over = weight + 0.1 * jnp.max(weight)

    def finish(m, carry):
        for p in range(2):
            at = pl.ds(pl.multiple_of((p * modes + m) * side, 8), side)
            new_probe_ref[p, m] = probe_ref[p, m].astype(jnp.float32) + sum_ref[at, :] / over
        return carry

    lax.fori_loop(0, modes, finish, 0)


def row_neighbours(x, z, near, deep):
    up = {"row_0": lax.rem(z + deep - (x == 0).astype(jnp.int32), deep), "row_1": lax.rem(x + near - 1, near)}
    down = {"row_0": lax.rem(z + (x == near - 1).astype(jnp.int32), deep), "row_1": lax.rem(x + 1, near)}
    return up, down


def halo_kernel(deep, near, obj_ref, cent_ref, ext_ref, cents_ref, send_sems, recv_sems):
    rows, cols = obj_ref.shape[1], obj_ref.shape[2]
    c, x, z = lax.axis_index("col"), lax.axis_index("row_1"), lax.axis_index("row_0")
    other = {"col": 1 - c}
    up, down = row_neighbours(x, z, near, deep)
    up_other, down_other = dict(up, **other), dict(down, **other)
    barrier = pltpu.get_barrier_semaphore()
    for peer in (other, up, down, up_other, down_other):
        pl.semaphore_signal(barrier, inc=1, device_id=peer, device_id_type=MESHID)
    pl.semaphore_wait(barrier, 5)
    tile = pl.ds(LANES, cols)
    first, last = Exchange(send_sems, recv_sems, 0), Exchange(send_sems, recv_sems, 8)
    edge = pl.ds(pl.multiple_of((1 - c) * (cols - LANES), LANES), LANES)
    held_edge = pl.ds(pl.multiple_of(LANES + (1 - c) * (cols - LANES), LANES), LANES)
    rim = pl.ds(pl.multiple_of(c * (cols + LANES), LANES), LANES)
    first.send(obj_ref, ext_ref.at[:, pl.ds(2 * rows, rows), tile], up)
    first.send(obj_ref, ext_ref.at[:, pl.ds(0, rows), tile], down)
    first.send(obj_ref.at[:, :, edge], ext_ref.at[:, pl.ds(rows, rows), rim], other)
    first.send(cent_ref, cents_ref.at[4 + c], up)
    first.send(cent_ref, cents_ref.at[4 + c], up_other)
    first.send(cent_ref, cents_ref.at[c], down)
    first.send(cent_ref, cents_ref.at[c], down_other)
    first.send(cent_ref, cents_ref.at[2 + c], other)
    cents_ref[2 + c] = cent_ref[...]
    ext_ref[:, pl.ds(rows, rows), tile] = obj_ref[...]
    ext_ref[:, :, rim] = jnp.zeros((2, 3 * rows, LANES), jnp.float32)
    for copy in first.copies[2:]:
        copy.wait()
    for i, start in ((0, 2 * rows), (1, 0)):
        first.copies[i].wait()
        here = pl.ds(start, rows)
        last.send(ext_ref.at[:, here, held_edge], ext_ref.at[:, here, rim], other)
    for copy in last.copies:
        copy.wait()

    @pl.when((x == 0) & (z == 0))
    def _():
        ext_ref[:, pl.ds(0, rows), :] = jnp.zeros((2, rows, cols + 2 * LANES), jnp.float32)

    @pl.when((x == near - 1) & (z == deep - 1))
    def _():
        ext_ref[:, pl.ds(2 * rows, rows), :] = jnp.zeros((2, rows, cols + 2 * LANES), jnp.float32)

def in_vmem(count):
    return [pl.BlockSpec(memory_space=pltpu.VMEM)] * count


def float_shapes(*shapes):
    return tuple(jax.ShapeDtypeStruct(shape, jnp.float32) for shape in shapes)


def local(obj_field, probe_modes, centers, amplitudes):
    _, tile_rows, tile_cols = obj_field.shape
    mode_count, side = probe_modes.shape[1:3]
    deep, near = lax.axis_size("row_0"), lax.axis_size("row_1")
    c, x, z = lax.axis_index("col"), lax.axis_index("row_1"), lax.axis_index("row_0")
    anchor = jnp.stack([(z * near + x) * tile_rows, c * tile_cols])
    cent = jnp.pad(centers - anchor, ((0, 7), (0, LANES - 2)))
    ext, cents = pl.pallas_call(
        functools.partial(halo_kernel, deep, near),
        out_shape=(
            jax.ShapeDtypeStruct((2, 3 * tile_rows, tile_cols + 2 * LANES), jnp.float32),
            jax.ShapeDtypeStruct((6, 8, LANES), jnp.int32),
        ),
        in_specs=in_vmem(2),
        out_specs=tuple(in_vmem(2)),
        scratch_shapes=[pltpu.SemaphoreType.DMA((16,)), pltpu.SemaphoreType.DMA((16,))],
        compiler_params=pltpu.CompilerParams(collective_id=1, has_side_effects=True, vmem_limit_bytes=VMEM_LIMIT),
        name="halo",
    )(obj_field, cent)
    row = z * near + x
    place = jnp.stack([c, c, (row > 0).astype(jnp.int32), (row < deep * near - 1).astype(jnp.int32)])
    cents = jnp.concatenate([cents[:, 0, :2], place.reshape(2, 2)], axis=0)
    planes = 2 * mode_count
    margin = side // 2
    wide = 3 * tile_cols + 2 * LANES
    sums, upd, illumination, top = pl.pallas_call(
        wave_kernel,
        out_shape=float_shapes(
            ((planes + 1) * side, side), (2, side, side), (tile_rows, tile_cols), (8, LANES)
        ),
        in_specs=[pl.BlockSpec(memory_space=pltpu.SMEM)] + in_vmem(5),
        out_specs=tuple(in_vmem(4)),
        scratch_shapes=[
            pltpu.VMEM((2, side, side), jnp.float32),
            pltpu.VMEM((mode_count, 2, side, side), jnp.float32),
            pltpu.VMEM((side, side), jnp.float32),
            pltpu.VMEM((tile_rows, wide), jnp.float32),
            pltpu.VMEM((side + 8, side), jnp.float32),
        ],
        compiler_params=pltpu.CompilerParams(vmem_limit_bytes=VMEM_LIMIT),
        name="waves",
    )(cents, ext, probe_modes, amplitudes, dft_tables(side), order_table(side))
    share = 4 * side
    chunks = ((planes * side, side),) + tuple(
        (start, share) for start in range(0, planes * side, share)
    )
    order = wave(len(chunks), *ORDER)
    sums, top, pair, part = all_sum(sums, top, upd, deep // NEAR, chunks, order)
    return pl.pallas_call(
        place_kernel,
        out_shape=float_shapes(obj_field.shape, probe_modes.shape),
        in_specs=[pl.BlockSpec(memory_space=pltpu.SMEM)] + in_vmem(8),
        out_specs=tuple(in_vmem(2)),
        scratch_shapes=[pltpu.VMEM((tile_rows, wide), jnp.float32), pltpu.VMEM((side + 8, side), jnp.float32)],
        compiler_params=pltpu.CompilerParams(vmem_limit_bytes=VMEM_LIMIT),
        name="place",
    )(cents, obj_field, probe_modes, upd, pair, part, illumination, top, sums)


def solution(mesh):
    split = Mesh(
        mesh.devices.reshape(mesh.shape["angle"], mesh.shape["row"] // 4, 4, mesh.shape["col"]),
        ("angle", "row_0", "row_1", "col"),
    )
    return jax.shard_map(
        local,
        mesh=split,
        in_specs=(
            P(None, ANGLE_ROW, "col"),
            P(),
            P(ANGLE_ROW_COL, None),
            P(ANGLE_ROW_COL, None, None),
        ),
        out_specs=(P(None, ANGLE_ROW, "col"), P(None, "angle", None, None)),
        check_vma=False,
    )
```

```python
import functools
import math

import jax
import jax.numpy as jnp
import numpy as np
from jax import lax
from jax.experimental import pallas as pl
from jax.experimental.pallas import tpu as pltpu
from jax.sharding import Mesh
from jax.sharding import PartitionSpec as P

ROW = ("row_0", "row_1")
ANGLE_ROW = ("angle", "row_0", "row_1")
ANGLE_ROW_COL = ("angle", "row_0", "row_1", "col")
MIB = 1024 * 1024
BEFORE_BARRIER = (0, 1)
ORDER = (
    (0, 0), (-1, 0), (1, 0), (2, 0), (-3, 2), (0, 1), (-1, 1), (1, 1), (2, 1), (3, 0),
    (0, 2), (-1, 2), (3, 1), (1, 2), (2, 2), (0, 3), (-1, 3), (3, 2), (0, 4), (-1, 4),
    (1, 3), (2, 3), (3, 3), (-2, 0), (1, 4), (2, 4), (3, 4), (0, 5), (-1, 5), (0, 6),
    (0, 7), (1, 5), (0, 8), (2, 5), (0, 9), (3, 5), (-2, 1), (1, 6), (2, 6), (1, 7),
    (3, 6), (2, 7), (1, 8), (3, 7), (2, 8), (1, 9), (3, 8), (2, 9), (3, 9), (-2, 2),
)

MESHID = pl.DeviceIdType.MESH
LANES = 128
NEAR = 4


class Exchange:
    def __init__(self, send_sems, recv_sems, first):
        self.send_sems, self.recv_sems, self.next = send_sems, recv_sems, first
        self.copies = []

    def send(self, src, dst, peer):
        copy = pltpu.make_async_remote_copy(
            src_ref=src,
            dst_ref=dst,
            send_sem=self.send_sems.at[self.next],
            recv_sem=self.recv_sems.at[self.next],
            device_id=peer,
            device_id_type=MESHID,
        )
        copy.start()
        self.next += 1
        self.copies.append(copy)


def rows_at(ref, start, size):
    return ref.at[pl.ds(pl.multiple_of(start, 8), size), :]


def far_order(count):
    return sorted(range(1, count), key=lambda d: -min(d, count - d))


COPIES_PER_CHUNK = 64


def all_sum_kernel(
    chunks, far, order, win_ref, probe_ref, amp_ref, tab_ref, order_ref, m_ref,
    o_ref, om_ref, upd_ref, pair_ref, part_ref, x_ref, waves, factor, *scratch,
):
    scratch = list(scratch)
    modes, side = probe_ref.shape[1], probe_ref.shape[2]
    send_sems, recv_sems = scratch[-2:]
    c, x, z = lax.axis_index("col"), lax.axis_index("row_1"), lax.axis_index("row_0")
    near_at, far_at = lax.rem(z, NEAR), lax.div(z, NEAR)
    partner = {"col": 1 - c}
    x_one = {"row_1": x + 1 - 2 * lax.rem(x, 2)}
    x_two = {"row_1": 3 - x}
    near_peers = {d: {"row_0": far_at * NEAR + lax.rem(near_at + d, NEAR)} for d in range(1, NEAR)}
    far_peers = {d: {"row_0": lax.rem(far_at + d, far) * NEAR + near_at} for d in range(1, far)}
    near_order, far_list = far_order(NEAR), far_order(far)
    barrier = pltpu.get_barrier_semaphore()
    up, down = row_neighbours(x, z, 4, far * NEAR)
    peers = [partner, x_one, x_two, up, down, *near_peers.values(), *far_peers.values()]
    for peer in peers:
        pl.semaphore_signal(barrier, inc=1, device_id=peer, device_id_type=MESHID)
    x_ref[pl.ds(2 * modes * side, side), :] = win_ref[0] * win_ref[0] + win_ref[1] * win_ref[1]
    upd_ref[...] = jnp.zeros_like(upd_ref)
    forward_waves(win_ref, probe_ref, amp_ref, tab_ref, order_ref, waves, factor)

    def modes_back(group):
        per = chunks[1][1] // (2 * side)
        backward_waves(group * per, per, win_ref, probe_ref, tab_ref, waves, factor, upd_ref, x_ref)

    for group in BEFORE_BARRIER:
        modes_back(group)
    pl.semaphore_wait(barrier, len(peers))

    mine, theirs = (
        pl.ds(pl.multiple_of(c * LANES, LANES), LANES),
        pl.ds(pl.multiple_of((1 - c) * LANES, LANES), LANES),
    )
    bit_a = lax.rem(lax.div(x + 1, 2), 2)
    bit_b = lax.div(x, 2)
    keep_one, peer_one = (bit_a, bit_b), (x_one, x_two)
    keep_two, peer_two = (bit_b, bit_a), (x_two, x_one)

    class Chunk:
        def __init__(self, index, start, rows, bufs):
            self.start, self.rows, self.bufs = start, rows, bufs
            self.next = index * COPIES_PER_CHUNK
            self.spread = rows // 128 >= 8
            self.pending = None

        def exchange(self):
            self.pending = Exchange(send_sems, recv_sems, self.next)
            return self.pending

        def arrive(self):
            for copy in self.pending.copies:
                copy.wait()
            self.next = self.pending.next

        def step(self, s):
            R, b = self.rows, self.bufs
            if s > 0:
                self.arrive()
            if s == 0:
                e = self.exchange()
                e.send(x_ref.at[pl.ds(self.start, R), theirs], b["rc"], partner)
            elif s == 1:
                b["s0"][...] = x_ref[pl.ds(self.start, R), mine] + b["rc"][...]
                e = self.exchange()
                for h in range(2):
                    src = rows_at(b["s0"], h * (R // 2) + (1 - keep_one[h]) * (R // 4), R // 4)
                    e.send(src, b["r1"].at[h], peer_one[h])
            elif s == 2:
                for h in range(2):
                    kept = pl.ds(pl.multiple_of(h * (R // 2) + keep_one[h] * (R // 4), 8), R // 4)
                    b["s1"][h] = b["s0"][kept, :] + b["r1"][h]
                e = self.exchange()
                for h in range(2):
                    src = rows_at(b["s1"].at[h], (1 - keep_two[h]) * (R // 8), R // 8)
                    e.send(src, b["r2"].at[h], peer_two[h])
            elif s == 3:
                for h in range(2):
                    kept = pl.ds(pl.multiple_of(keep_two[h] * (R // 8), 8), R // 8)
                    b["s2"][pl.ds(h * (R // 8), R // 8), :] = b["s1"][h, kept, :] + b["r2"][h]
                e = self.exchange()
                for d in near_order:
                    src = rows_at(b["s2"], lax.rem(near_at + d, NEAR) * (R // 16), R // 16)
                    e.send(src, b["r3"].at[d - 1], near_peers[d])
            elif s == 4:
                kept = pl.ds(pl.multiple_of(near_at * (R // 16), 8), R // 16)
                total = b["s2"][kept, :]
                for d in range(1, NEAR):
                    total = total + b["r3"][d - 1]
                b["s3"][...] = total
                e = self.exchange()
                for d in far_list:
                    if self.spread:
                        src = rows_at(b["s3"], lax.rem(far_at + d, far) * (R // 128), R // 128)
                    else:
                        src = b["s3"]
                    e.send(src, b["r4"].at[d - 1], far_peers[d])
            elif s == 5:
                if self.spread:
                    at = pl.ds(pl.multiple_of(far_at * (R // 128), 8), R // 128)
                    total = b["s3"][at, :]
                    for d in range(1, far):
                        total = total + b["r4"][d - 1]
                    b["g3"][at, :] = total
                    e = self.exchange()
                    block = rows_at(b["g3"], far_at * (R // 128), R // 128)
                    for d in far_list:
                        e.send(block, block, far_peers[d])
                else:
                    b["r4"][far - 1] = b["s3"][...]
                    total = jnp.zeros((R // 16, LANES), jnp.float32)
                    for owner in range(far):
                        total = total + b["r4"][lax.rem(far_at - owner + far - 1, far)]
                    b["g3"][...] = total
                    self.exchange()
            elif s == 6:
                at = pl.ds(pl.multiple_of(near_at * (R // 16), 8), R // 16)
                e = self.exchange()
                dst = rows_at(b["g2"], near_at * (R // 16), R // 16)
                for d in near_order:
                    e.send(b["g3"], dst, near_peers[d])
                b["g2"][at, :] = b["g3"][...]
            elif s == 7:
                e = self.exchange()
                for h in range(2):
                    src = rows_at(b["g2"], h * (R // 8), R // 8)
                    dst = rows_at(b["g1"].at[h], keep_two[h] * (R // 8), R // 8)
                    e.send(src, dst, peer_two[h])
                for h in range(2):
                    at = pl.ds(pl.multiple_of(keep_two[h] * (R // 8), 8), R // 8)
                    b["g1"][h, at, :] = b["g2"][pl.ds(h * (R // 8), R // 8), :]
            elif s == 8:
                e = self.exchange()
                for h in range(2):
                    dst = rows_at(b["g0"], h * (R // 2) + keep_one[h] * (R // 4), R // 4)
                    e.send(b["g1"].at[h], dst, peer_one[h])
                for h in range(2):
                    at = pl.ds(pl.multiple_of(h * (R // 2) + keep_one[h] * (R // 4), 8), R // 4)
                    b["g0"][at, :] = b["g1"][h]
            elif s == 9:
                e = self.exchange()
                e.send(b["g0"], o_ref.at[pl.ds(self.start, R), mine], partner)
                o_ref[pl.ds(self.start, R), mine] = b["g0"][...]

    class Peak:
        def __init__(self, index, bufs):
            self.next, self.bufs = index * COPIES_PER_CHUNK, bufs
            self.stages = [[partner], [x_one], [x_two], list(near_peers.values()), list(far_peers.values())]
            self.slot = 0
            self.copies = []

        def step(self, s):
            held, came = self.bufs["held"], self.bufs["came"]
            if s > 0:
                top = m_ref[...] if s == 1 else held[s - 1]
                for i, copy in enumerate(self.copies):
                    copy.wait()
                    top = jnp.maximum(top, came[self.slot - len(self.copies) + i])
                if s == 5:
                    om_ref[...] = top
                    return
                held[s] = top
            e = Exchange(send_sems, recv_sems, self.next)
            for peer in self.stages[s]:
                e.send(m_ref if s == 0 else held.at[s], came.at[self.slot], peer)
                self.slot += 1
            self.next, self.copies = e.next, e.copies

    class Fold:
        def __init__(self, index):
            self.index = index

        def step(self, s):
            half = upd_ref.shape[1] // 2
            if s == 0:
                self.first = Exchange(send_sems, recv_sems, self.index * COPIES_PER_CHUNK)
                self.first.send(upd_ref.at[:, pl.ds(half, half), :], part_ref.at[0, c], down)
                self.first.send(upd_ref.at[:, pl.ds(0, half), :], part_ref.at[1, c], up)
                self.first.send(upd_ref, pair_ref, partner)
            elif s == 1:
                self.last = Exchange(send_sems, recv_sems, self.index * COPIES_PER_CHUNK + 8)
                for i in range(2):
                    self.first.copies[i].wait()
                    self.last.send(part_ref.at[i, c], part_ref.at[i, c], partner)
                self.first.copies[2].wait()
            else:
                for copy in self.last.copies:
                    copy.wait()

    fold = Fold(len(chunks) + 1)
    objects = []
    at = 0
    for i, (start, rows) in enumerate(chunks):
        names = chunk_buffers(rows, far)
        bufs = dict(zip(names, scratch[at : at + len(names)]))
        at += len(names)
        objects.append(Chunk(i, start, rows, bufs))
    peak = Peak(len(chunks), dict(held=scratch[at], came=scratch[at + 1]))
    for which, s in order:
        if which == -1:
            peak.step(s)
        elif which == -2:
            fold.step(s)
        elif which == -3:
            modes_back(s)
        else:
            objects[which].step(s)
    for o in objects:
        o.arrive()


def chunk_buffers(rows, far):
    R = rows
    last = R // 128 if R // 128 >= 8 else R // 16
    return dict(
        rc=(R, LANES), s0=(R, LANES), r1=(2, R // 4, LANES), s1=(2, R // 4, LANES), r2=(2, R // 8, LANES),
        s2=(R // 4, LANES), r3=(NEAR - 1, R // 16, LANES), s3=(R // 16, LANES), r4=(far, last, LANES),
        g3=(R // 16, LANES), g2=(R // 4, LANES), g1=(2, R // 4, LANES), g0=(R, LANES),
    )


def all_sum(win, probe, amp, m, far, chunks, order):
    bufs = []
    for _, rows in chunks:
        bufs += [pltpu.VMEM(s, jnp.float32) for s in chunk_buffers(rows, far).values()]
    bufs += [pltpu.VMEM((6, 8, LANES), jnp.float32), pltpu.VMEM((3 + NEAR - 1 + far - 1, 8, LANES), jnp.float32)]
    count = COPIES_PER_CHUNK * (len(chunks) + 2)
    modes, side = probe.shape[1:3]
    rows = (2 * modes + 1) * side
    shapes = ((rows, side), m.shape, win.shape, win.shape, (2, 2, 2, side // 2, side))
    bufs = [
        pltpu.VMEM((rows, side), jnp.float32),
        pltpu.VMEM((modes, 2, side, side), jnp.float32),
        pltpu.VMEM((side, side), jnp.float32),
    ] + bufs
    return pl.pallas_call(
        functools.partial(all_sum_kernel, chunks, far, order),
        out_shape=tuple(jax.ShapeDtypeStruct(shape, jnp.float32) for shape in shapes),
        in_specs=[pl.BlockSpec(memory_space=pltpu.VMEM)] * 6,
        out_specs=(pl.BlockSpec(memory_space=pltpu.VMEM),) * 5,
        scratch_shapes=bufs + [pltpu.SemaphoreType.DMA((count,)), pltpu.SemaphoreType.DMA((count,))],
        compiler_params=pltpu.CompilerParams(collective_id=0, has_side_effects=True, vmem_limit_bytes=30 * MIB),
        name="all_sum",
    )(win, probe, amp, dft_tables(side), order_table(side), m)


def dft_tables(side):
    half = side // 2
    n, q = np.arange(half)[None, :], np.arange(half)[:, None]
    tables = []
    for odd in range(2):
        phase = 2.0 * np.pi * ((n * (2 * q + odd)) % side) / side
        cosine, sine = np.cos(phase) / math.sqrt(side), np.sin(phase) / math.sqrt(side)
        table = np.block([[cosine, sine], [-sine, cosine]])
        tables += [table, table.T]
    tables = np.stack(tables).astype(np.float32)
    high = tables.astype(jnp.bfloat16)
    low = (tables - high.astype(np.float32)).astype(jnp.bfloat16)
    return np.stack([high, low], axis=1)


def order_table(side):
    table = np.zeros((side, side), np.float32)
    at = np.arange(side)
    table[at, np.where(at < side // 2, 2 * at, 2 * at + 1 - side)] = 1.0
    return table.astype(jnp.bfloat16)


def halves(value):
    high = value.astype(jnp.bfloat16)
    return high, (value - high.astype(jnp.float32)).astype(jnp.bfloat16)


def dot(a, b):
    return jnp.dot(a, b, preferred_element_type=jnp.float32)


def from_left(tab_ref, which, value):
    high, low = halves(value)
    return dot(tab_ref[which, 0], high) + dot(tab_ref[which, 0], low) + dot(tab_ref[which, 1], high)


def from_right(tab_ref, which, value):
    high, low = halves(value)
    return dot(high, tab_ref[which, 0]) + dot(low, tab_ref[which, 0]) + dot(high, tab_ref[which, 1])


def to_far_field(tab_ref, re, im):
    h = re.shape[0] // 2
    plus = jnp.concatenate([re[:h] + re[h:], im[:h] + im[h:]], axis=0)
    minus = jnp.concatenate([re[:h] - re[h:], im[:h] - im[h:]], axis=0)
    even, odd = from_left(tab_ref, 0, plus), from_left(tab_ref, 2, minus)
    re = jnp.concatenate([even[:h], odd[:h]], axis=0)
    im = jnp.concatenate([even[h:], odd[h:]], axis=0)
    plus = jnp.concatenate([re[:, :h] + re[:, h:], im[:, :h] + im[:, h:]], axis=1)
    minus = jnp.concatenate([re[:, :h] - re[:, h:], im[:, :h] - im[:, h:]], axis=1)
    even, odd = from_right(tab_ref, 1, plus), from_right(tab_ref, 3, minus)
    re = jnp.concatenate([even[:, :h], odd[:, :h]], axis=1)
    im = jnp.concatenate([even[:, h:], odd[:, h:]], axis=1)
    return re, im


def from_far_field(tab_ref, re, im):
    h = re.shape[0] // 2
    even = from_right(tab_ref, 0, jnp.concatenate([re[:, :h], im[:, :h]], axis=1))
    odd = from_right(tab_ref, 2, jnp.concatenate([re[:, h:], im[:, h:]], axis=1))
    plus, minus = even + odd, even - odd
    re = jnp.concatenate([plus[:, :h], minus[:, :h]], axis=1)
    im = jnp.concatenate([plus[:, h:], minus[:, h:]], axis=1)
    even = from_left(tab_ref, 1, jnp.concatenate([re[:h], im[:h]], axis=0))
    odd = from_left(tab_ref, 3, jnp.concatenate([re[h:], im[h:]], axis=0))
    plus, minus = even + odd, even - odd
    re = jnp.concatenate([plus[:h], minus[:h]], axis=0)
    im = jnp.concatenate([plus[h:], minus[h:]], axis=0)
    return re, im


def reorder(order_ref, value):
    def three(v):
        high, rest = v.astype(jnp.bfloat16), None
        rest = v - high.astype(jnp.float32)
        middle = rest.astype(jnp.bfloat16)
        return high, middle, (rest - middle.astype(jnp.float32)).astype(jnp.bfloat16)

    table = order_ref[...]
    high, middle, low = three(value)
    value = dot(table, high) + dot(table, middle) + dot(table, low)
    across = lambda v: lax.dot_general(
        v, table, (((1,), (1,)), ((), ())), preferred_element_type=jnp.float32
    )
    high, middle, low = three(value)
    return across(high) + across(middle) + across(low)


def from_row(ref, row, rows, cols):
    off = lax.rem(row, 8)
    value = ref[pl.ds(pl.multiple_of(row - off, 8), rows + 8), cols]
    return pltpu.roll(value, lax.rem(rows + 8 - off, rows + 8), 0)[:rows]


def add_window(acc_ref, source_ref, row, col, scale=None):
    rows = acc_ref.shape[0]
    side = source_ref.shape[1]
    value = from_row(source_ref, row, rows, slice(None))
    if scale is not None:
        value = jnp.where(scale > 0, value, 0.0)
    value = jnp.concatenate([value, jnp.zeros((rows, LANES), jnp.float32)], axis=1)
    value = pltpu.roll(value, lax.rem(col, LANES), 1)
    at = pl.ds(pl.multiple_of(lax.div(col, LANES) * LANES, LANES), side + LANES)
    acc_ref[:, at] = acc_ref[:, at] + value


def sources(cent_ref, tile_cols, margin):
    c = cent_ref[6, 0]
    for where in range(3):
        for side_col in range(2):
            k = where * 2 + side_col
            row = margin - cent_ref[k, 0]
            col = (side_col - c) * tile_cols + cent_ref[k, 1] - margin + tile_cols + margin
            there = jnp.int32(1)
            if where == 0:
                there = cent_ref[7, 0]
            if where == 2:
                there = cent_ref[7, 1]
            yield where, side_col, row, col, there


def forward_waves(win, probe_ref, amp_ref, tab_ref, order_ref, far, amp):
    amp[...] = jnp.zeros_like(amp)

    def forward(m, carry):
        pr, pi = probe_ref[0, m].astype(jnp.float32), probe_ref[1, m].astype(jnp.float32)
        re, im = to_far_field(tab_ref, pr * win[0] - pi * win[1], pr * win[1] + pi * win[0])
        far[m, 0], far[m, 1] = re, im
        amp[...] += re * re + im * im
        return carry

    lax.fori_loop(0, probe_ref.shape[1], forward, 0)
    amp[...] = reorder(order_ref, amp_ref[0]) / (jnp.sqrt(amp[...]) + 0.5)


def backward_waves(first, count, win, probe_ref, tab_ref, far, amp, upd_ref, sum_ref):
    side = probe_ref.shape[2]

    def backward(m, carry):
        factor = amp[...]
        re, im = from_far_field(tab_ref, far[m, 0] * factor, far[m, 1] * factor)
        pr, pi = probe_ref[0, m].astype(jnp.float32), probe_ref[1, m].astype(jnp.float32)
        wr, wi = win[0], win[1]
        re = re - (pr * wr - pi * wi)
        im = im - (pr * wi + pi * wr)
        upd_ref[0] += pr * re + pi * im
        upd_ref[1] += pr * im - pi * re
        at_re, at_im = pl.multiple_of(2 * m * side, 8), pl.multiple_of((2 * m + 1) * side, 8)
        sum_ref[pl.ds(at_re, side), :] = wr * re + wi * im
        sum_ref[pl.ds(at_im, side), :] = wr * im - wi * re
        return carry

    lax.fori_loop(first, first + count, backward, 0)


def window_kernel(cent_ref, ext_ref, probe_ref, win_ref, illum_ref, top_ref, acc, shifted):
    modes, side = probe_ref.shape[1], probe_ref.shape[2]
    margin = side // 2
    tile_rows, tile_cols = illum_ref.shape
    c = cent_ref[6, 0]
    own_row, own_col = cent_ref[2 + c, 0], cent_ref[2 + c, 1]
    shift = lax.rem(own_col, LANES)
    at = pl.ds(pl.multiple_of(own_col - shift, LANES), side + LANES)
    for p in range(2):
        value = from_row(ext_ref.at[p], own_row, side, at)
        value = pltpu.roll(value, lax.rem(side + LANES - shift, side + LANES), 1)
        win_ref[p] = value[:, :side]
    spot = jnp.zeros((side, side), jnp.float32)
    for m in range(modes):
        pr, pi = probe_ref[0, m].astype(jnp.float32), probe_ref[1, m].astype(jnp.float32)
        spot = spot + (pr * pr + pi * pi)
    shifted[pl.ds(0, side), :] = spot
    zeros = jnp.zeros((margin, side), jnp.float32)
    spot_top, spot_bottom = shifted[pl.ds(0, margin), :], shifted[pl.ds(margin, margin), :]
    acc[...] = jnp.zeros_like(acc)
    laid = {0: (spot_bottom, zeros), 1: (spot_top, spot_bottom), 2: (zeros, spot_top)}
    for where, side_col, row, col, there in sources(cent_ref, tile_cols, margin):
        if side_col == 0:
            shifted[pl.ds(0, margin), :], shifted[pl.ds(margin, margin), :] = laid[where]
        add_window(acc, shifted, row, col, there)
    total = acc[:, pl.ds(tile_cols + margin, tile_cols)]
    illum_ref[...] = total
    top_ref[...] = jnp.full(top_ref.shape, jnp.max(total))


def place_kernel(
    cent_ref, obj_ref, probe_ref, upd_ref, pair_ref, part_ref, illum_ref, top_ref, sum_ref,
    new_obj_ref, new_probe_ref, acc, shifted,
):
    modes, side = probe_ref.shape[1], probe_ref.shape[2]
    margin = side // 2
    tile_cols = illum_ref.shape[1]
    c = cent_ref[6, 0]
    below = illum_ref[...] + 0.1 * jnp.max(top_ref[...])
    for p in range(2):
        acc[...] = jnp.zeros_like(acc)
        for where, side_col, row, col, there in sources(cent_ref, tile_cols, margin):
            if where == 1:
                shifted[pl.ds(0, side), :] = jnp.where(c == side_col, upd_ref[p], pair_ref[p])
            else:
                part = part_ref[where // 2, side_col, p]
                first = where // 2 * margin
                shifted[pl.ds(first, margin), :] = part
                shifted[pl.ds(margin - first, margin), :] = jnp.zeros((margin, side), jnp.float32)
            add_window(acc, shifted, row, col, there)
        new_obj_ref[p] = obj_ref[p] + acc[:, pl.ds(tile_cols + margin, tile_cols)] / below
    weight = sum_ref[pl.ds(2 * modes * side, side), :]
    over = weight + 0.1 * jnp.max(weight)

    def finish(m, carry):
        for p in range(2):
            at = pl.ds(pl.multiple_of((2 * m + p) * side, 8), side)
            new_probe_ref[p, m] = probe_ref[p, m].astype(jnp.float32) + sum_ref[at, :] / over
        return carry

    lax.fori_loop(0, modes, finish, 0)


def row_neighbours(x, z, near, deep):
    up = {"row_0": lax.rem(z + deep - (x == 0).astype(jnp.int32), deep), "row_1": lax.rem(x + near - 1, near)}
    down = {"row_0": lax.rem(z + (x == near - 1).astype(jnp.int32), deep), "row_1": lax.rem(x + 1, near)}
    return up, down


def halo_kernel(deep, near, obj_ref, cent_ref, ext_ref, cents_ref, send_sems, recv_sems):
    rows, cols = obj_ref.shape[1], obj_ref.shape[2]
    c, x, z = lax.axis_index("col"), lax.axis_index("row_1"), lax.axis_index("row_0")
    other = {"col": 1 - c}
    up, down = row_neighbours(x, z, near, deep)
    up_other, down_other = dict(up, **other), dict(down, **other)
    barrier = pltpu.get_barrier_semaphore()
    for peer in (other, up, down, up_other, down_other):
        pl.semaphore_signal(barrier, inc=1, device_id=peer, device_id_type=MESHID)
    pl.semaphore_wait(barrier, 5)
    tile = pl.ds(LANES, cols)
    first, last = Exchange(send_sems, recv_sems, 0), Exchange(send_sems, recv_sems, 8)
    edge = pl.ds(pl.multiple_of((1 - c) * (cols - LANES), LANES), LANES)
    held_edge = pl.ds(pl.multiple_of(LANES + (1 - c) * (cols - LANES), LANES), LANES)
    rim = pl.ds(pl.multiple_of(c * (cols + LANES), LANES), LANES)
    first.send(obj_ref, ext_ref.at[:, pl.ds(2 * rows, rows), tile], up)
    first.send(obj_ref, ext_ref.at[:, pl.ds(0, rows), tile], down)
    first.send(obj_ref.at[:, :, edge], ext_ref.at[:, pl.ds(rows, rows), rim], other)
    first.send(cent_ref, cents_ref.at[4 + c], up)
    first.send(cent_ref, cents_ref.at[4 + c], up_other)
    first.send(cent_ref, cents_ref.at[c], down)
    first.send(cent_ref, cents_ref.at[c], down_other)
    first.send(cent_ref, cents_ref.at[2 + c], other)
    cents_ref[2 + c] = cent_ref[...]
    ext_ref[:, pl.ds(rows, rows), tile] = obj_ref[...]
    ext_ref[:, :, rim] = jnp.zeros((2, 3 * rows, LANES), jnp.float32)
    for copy in first.copies[2:]:
        copy.wait()
    for i, start in ((0, 2 * rows), (1, 0)):
        first.copies[i].wait()
        here = pl.ds(start, rows)
        last.send(ext_ref.at[:, here, held_edge], ext_ref.at[:, here, rim], other)
    for copy in last.copies:
        copy.wait()

    @pl.when((x == 0) & (z == 0))
    def _():
        ext_ref[:, pl.ds(0, rows), :] = jnp.zeros((2, rows, cols + 2 * LANES), jnp.float32)

    @pl.when((x == near - 1) & (z == deep - 1))
    def _():
        ext_ref[:, pl.ds(2 * rows, rows), :] = jnp.zeros((2, rows, cols + 2 * LANES), jnp.float32)

def in_vmem(count):
    return [pl.BlockSpec(memory_space=pltpu.VMEM)] * count


def float_shapes(*shapes):
    return tuple(jax.ShapeDtypeStruct(shape, jnp.float32) for shape in shapes)


def local(obj_field, probe_modes, centers, amplitudes):
    _, tile_rows, tile_cols = obj_field.shape
    mode_count, side = probe_modes.shape[1:3]
    deep, near = lax.axis_size("row_0"), lax.axis_size("row_1")
    c, x, z = lax.axis_index("col"), lax.axis_index("row_1"), lax.axis_index("row_0")
    anchor = jnp.stack([(z * near + x) * tile_rows, c * tile_cols])
    cent = jnp.pad(centers - anchor, ((0, 7), (0, LANES - 2)))
    ext, cents = pl.pallas_call(
        functools.partial(halo_kernel, deep, near),
        out_shape=(
            jax.ShapeDtypeStruct((2, 3 * tile_rows, tile_cols + 2 * LANES), jnp.float32),
            jax.ShapeDtypeStruct((6, 8, LANES), jnp.int32),
        ),
        in_specs=in_vmem(2),
        out_specs=tuple(in_vmem(2)),
        scratch_shapes=[pltpu.SemaphoreType.DMA((16,)), pltpu.SemaphoreType.DMA((16,))],
        compiler_params=pltpu.CompilerParams(collective_id=1, has_side_effects=True, vmem_limit_bytes=6 * MIB),
        name="halo",
    )(obj_field, cent)
    row = z * near + x
    place = jnp.stack([c, c, (row > 0).astype(jnp.int32), (row < deep * near - 1).astype(jnp.int32)])
    cents = jnp.concatenate([cents[:, 0, :2], place.reshape(2, 2)], axis=0)
    planes = 2 * mode_count
    margin = side // 2
    wide = 3 * tile_cols + 2 * LANES
    win, illumination, top = pl.pallas_call(
        window_kernel,
        out_shape=float_shapes((2, side, side), (tile_rows, tile_cols), (8, LANES)),
        in_specs=[pl.BlockSpec(memory_space=pltpu.SMEM)] + in_vmem(2),
        out_specs=tuple(in_vmem(3)),
        scratch_shapes=[pltpu.VMEM((tile_rows, wide), jnp.float32), pltpu.VMEM((side + 8, side), jnp.float32)],
        compiler_params=pltpu.CompilerParams(vmem_limit_bytes=8 * MIB),
        name="window",
    )(cents, ext, probe_modes)
    share = 4 * side
    chunks = ((planes * side, side),) + tuple(
        (start, share) for start in range(0, planes * side, share)
    )
    sums, top, upd, pair, part = all_sum(win, probe_modes, amplitudes, top, deep // NEAR, chunks, ORDER)
    return pl.pallas_call(
        place_kernel,
        out_shape=float_shapes(obj_field.shape, probe_modes.shape),
        in_specs=[pl.BlockSpec(memory_space=pltpu.SMEM)] + in_vmem(8),
        out_specs=tuple(in_vmem(2)),
        scratch_shapes=[pltpu.VMEM((tile_rows, wide), jnp.float32), pltpu.VMEM((side + 8, side), jnp.float32)],
        compiler_params=pltpu.CompilerParams(vmem_limit_bytes=16 * MIB),
        name="place",
    )(cents, obj_field, probe_modes, upd, pair, part, illumination, top, sums)


def solution(mesh):
    split = Mesh(
        mesh.devices.reshape(mesh.shape["angle"], mesh.shape["row"] // 4, 4, mesh.shape["col"]),
        ("angle", "row_0", "row_1", "col"),
    )
    return jax.shard_map(
        local,
        mesh=split,
        in_specs=(
            P(None, ANGLE_ROW, "col"),
            P(),
            P(ANGLE_ROW_COL, None),
            P(ANGLE_ROW_COL, None, None),
        ),
        out_specs=(P(None, ANGLE_ROW, "col"), P(None, "angle", None, None)),
        check_vma=False,
    )
```

```python
import functools
import math

import jax
import jax.numpy as jnp
import numpy as np
from jax import lax
from jax.experimental import pallas as pl
from jax.experimental.pallas import tpu as pltpu
from jax.sharding import Mesh
from jax.sharding import PartitionSpec as P

ROW = ("row_0", "row_1")
ANGLE_ROW = ("angle", "row_0", "row_1")
ANGLE_ROW_COL = ("angle", "row_0", "row_1", "col")
MIB = 1024 * 1024
BEFORE_BARRIER = (0, 1)
ORDER = (
    (1, 0), (2, 0), (1, 1), (2, 1), (-3, 2), (3, 0), (0, 0), (-1, 0), (1, 2), (3, 1),
    (2, 2), (1, 3), (0, 1), (-1, 1), (3, 2), (1, 4), (2, 3), (0, 2), (-1, 2), (3, 3),
    (2, 4), (0, 3), (-1, 3), (1, 5), (0, 4), (-1, 4), (-2, 0), (3, 4), (2, 5), (3, 5),
    (0, 5), (-1, 5), (1, 6), (2, 6), (-2, 1), (3, 6), (0, 6), (-1, 6), (1, 7), (1, 8),
    (2, 7), (1, 9), (3, 7), (2, 8), (1, 10), (0, 7), (3, 8), (2, 9), (0, 8), (3, 9),
    (0, 9), (2, 10), (1, 11), (-2, 2), (3, 10), (2, 11), (0, 10), (3, 11), (0, 11),
)

MESHID = pl.DeviceIdType.MESH
LANES = 128
NEAR = 4


class Exchange:
    def __init__(self, send_sems, recv_sems, first):
        self.send_sems, self.recv_sems, self.next = send_sems, recv_sems, first
        self.copies = []

    def send(self, src, dst, peer):
        copy = pltpu.make_async_remote_copy(
            src_ref=src,
            dst_ref=dst,
            send_sem=self.send_sems.at[self.next],
            recv_sem=self.recv_sems.at[self.next],
            device_id=peer,
            device_id_type=MESHID,
        )
        copy.start()
        self.next += 1
        self.copies.append(copy)


def rows_at(ref, start, size):
    return ref.at[pl.ds(pl.multiple_of(start, 8), size), :]


def far_order(count):
    return sorted(range(1, count), key=lambda d: -min(d, count - d))


COPIES_PER_CHUNK = 64


def all_sum_kernel(
    chunks, far, order, win_ref, probe_ref, amp_ref, tab_ref, order_ref, m_ref,
    o_ref, om_ref, upd_ref, pair_ref, part_ref, x_ref, waves, factor, *scratch,
):
    scratch = list(scratch)
    modes, side = probe_ref.shape[1], probe_ref.shape[2]
    send_sems, recv_sems = scratch[-2:]
    c, x, z = lax.axis_index("col"), lax.axis_index("row_1"), lax.axis_index("row_0")
    far_at, deep = lax.div(z, NEAR), far * NEAR
    partner = {"col": 1 - c}
    x_one = {"row_1": x + 1 - 2 * lax.rem(x, 2)}
    x_two = {"row_1": 3 - x}
    bit_a = lax.rem(lax.div(x + 1, 2), 2)
    bit_b = lax.div(x, 2)
    halvings = [((x_one, bit_a), (x_two, bit_b)), ((x_two, bit_b), (x_one, bit_a))]
    for reach in (1, 2):
        pairs = []
        for shift in (0, NEAR - 1):
            at = lax.rem(z + shift, NEAR)
            bit = lax.rem(lax.div(at, reach), 2)
            pairs.append(({"row_0": lax.rem(z + deep + reach - 2 * reach * bit, deep)}, bit))
        halvings.append(tuple(pairs))
    near_peers = [peer for level in halvings[2:] for peer, _ in level]
    far_peers = {d: {"row_0": lax.rem(far_at + d, far) * NEAR + lax.rem(z, NEAR)} for d in range(1, far)}
    far_list = far_order(far)
    barrier = pltpu.get_barrier_semaphore()
    up, down = row_neighbours(x, z, 4, deep)
    peers = [partner, x_one, x_two, up, down, *near_peers, *far_peers.values()]
    for peer in peers:
        pl.semaphore_signal(barrier, inc=1, device_id=peer, device_id_type=MESHID)
    x_ref[pl.ds(2 * modes * side, side), :] = win_ref[0] * win_ref[0] + win_ref[1] * win_ref[1]
    upd_ref[...] = jnp.zeros_like(upd_ref)
    forward_waves(win_ref, probe_ref, amp_ref, tab_ref, order_ref, waves, factor)

    def modes_back(group):
        per = chunks[1][1] // (2 * side)
        backward_waves(group * per, per, win_ref, probe_ref, tab_ref, waves, factor, upd_ref, x_ref)

    for group in BEFORE_BARRIER:
        modes_back(group)
    pl.semaphore_wait(barrier, len(peers))

    mine, theirs = (
        pl.ds(pl.multiple_of(c * LANES, LANES), LANES),
        pl.ds(pl.multiple_of((1 - c) * LANES, LANES), LANES),
    )

    class Chunk:
        def __init__(self, index, start, rows, bufs):
            self.start, self.rows, self.bufs = start, rows, bufs
            self.next = index * COPIES_PER_CHUNK
            self.whole = rows // 128 >= 8
            self.pending = None

        def exchange(self):
            self.pending = Exchange(send_sems, recv_sems, self.next)
            return self.pending

        def arrive(self):
            for copy in self.pending.copies:
                copy.wait()
            self.next = self.pending.next

        def held(self, name, level, h):
            ref = self.bufs[name + str(level)]
            return ref.at[pl.ds(h * (self.rows // 2), self.rows // 2), :] if level == 0 else ref.at[h]

        def tile_of(self, name, owner):
            half_group = far // 2
            first = lax.rem(owner, half_group) * 8 if self.whole else 0
            return self.bufs[name].at[lax.div(owner, half_group)].at[pl.ds(pl.multiple_of(first, 8), 8), :]

        def step(self, s):
            R, b, steps = self.rows, self.bufs, len(halvings)
            if s > 0:
                self.arrive()
            e = self.exchange()
            if s == 0:
                e.send(x_ref.at[pl.ds(self.start, R), theirs], b["rc"], partner)
            elif s <= steps:
                level = s - 1
                if level == 0:
                    b["s0"][...] = x_ref[pl.ds(self.start, R), mine] + b["rc"][...]
                else:
                    self.add(level)
                size = R >> (level + 2)
                for h in range(2):
                    peer, keep = halvings[level][h]
                    e.send(rows_at(self.held("s", level, h), (1 - keep) * size, size), b["r" + str(level)].at[h], peer)
            elif s == steps + 1:
                self.add(steps)
                for d in far_list:
                    src = self.tile_of("s" + str(steps), lax.rem(far_at + d, far))
                    e.send(src, b["rf"].at[d - 1], far_peers[d])
            elif s == steps + 2:
                own = self.tile_of("s" + str(steps), far_at)
                block = self.tile_of("g" + str(steps), far_at)
                if self.whole:
                    total = own[...]
                    for d in range(1, far):
                        total = total + b["rf"][d - 1]
                    block[...] = total
                    for d in far_list:
                        e.send(block, block, far_peers[d])
                else:
                    b["rf"][far - 1] = own[...]
                    total = jnp.zeros((8, LANES), jnp.float32)
                    for owner in range(far):
                        total = total + b["rf"][lax.rem(far_at - owner + far - 1 + far, far)]
                    block[...] = total
                    e.send(block, block, far_peers[far // 2])
            elif s <= 2 * steps + 2:
                level = 2 * steps + 2 - s
                size = R >> (level + 2)
                for h in range(2):
                    peer, keep = halvings[level][h]
                    target = rows_at(self.held("g", level, h), keep * size, size)
                    e.send(self.held("g", level + 1, h), target, peer)
                for h in range(2):
                    _, keep = halvings[level][h]
                    target = rows_at(self.held("g", level, h), keep * size, size)
                    target[...] = self.held("g", level + 1, h)[...]
            else:
                e.send(b["g0"], o_ref.at[pl.ds(self.start, R), mine], partner)
                o_ref[pl.ds(self.start, R), mine] = b["g0"][...]

        def add(self, level):
            size = self.rows >> (level + 1)
            for h in range(2):
                _, keep = halvings[level - 1][h]
                kept = rows_at(self.held("s", level - 1, h), keep * size, size)
                self.bufs["s" + str(level)][h] = kept[...] + self.bufs["r" + str(level - 1)][h]

    class Peak:
        def __init__(self, index, bufs):
            self.next, self.bufs = index * COPIES_PER_CHUNK, bufs
            self.stages = [[partner], *[[level[0][0]] for level in halvings], list(far_peers.values())]
            self.slot = 0
            self.copies = []

        def step(self, s):
            held, came = self.bufs["held"], self.bufs["came"]
            if s > 0:
                top = m_ref[...] if s == 1 else held[s - 1]
                for i, copy in enumerate(self.copies):
                    copy.wait()
                    top = jnp.maximum(top, came[self.slot - len(self.copies) + i])
                if s == len(self.stages):
                    om_ref[...] = top
                    return
                held[s] = top
            e = Exchange(send_sems, recv_sems, self.next)
            for peer in self.stages[s]:
                e.send(m_ref if s == 0 else held.at[s], came.at[self.slot], peer)
                self.slot += 1
            self.next, self.copies = e.next, e.copies

    class Fold:
        def __init__(self, index):
            self.index = index

        def step(self, s):
            half = upd_ref.shape[1] // 2
            if s == 0:
                self.first = Exchange(send_sems, recv_sems, self.index * COPIES_PER_CHUNK)
                self.first.send(upd_ref.at[:, pl.ds(half, half), :], part_ref.at[0, c], down)
                self.first.send(upd_ref.at[:, pl.ds(0, half), :], part_ref.at[1, c], up)
                self.first.send(upd_ref, pair_ref, partner)
            elif s == 1:
                self.last = Exchange(send_sems, recv_sems, self.index * COPIES_PER_CHUNK + 8)
                for i in range(2):
                    self.first.copies[i].wait()
                    self.last.send(part_ref.at[i, c], part_ref.at[i, c], partner)
                self.first.copies[2].wait()
            else:
                for copy in self.last.copies:
                    copy.wait()

    fold = Fold(len(chunks) + 1)
    objects = []
    at = 0
    for i, (start, rows) in enumerate(chunks):
        names = chunk_buffers(rows, far)
        bufs = dict(zip(names, scratch[at : at + len(names)]))
        at += len(names)
        objects.append(Chunk(i, start, rows, bufs))
    peak = Peak(len(chunks), dict(held=scratch[at], came=scratch[at + 1]))
    for which, s in order:
        if which == -1:
            peak.step(s)
        elif which == -2:
            fold.step(s)
        elif which == -3:
            modes_back(s)
        else:
            objects[which].step(s)
    for o in objects:
        o.arrive()


def chunk_buffers(rows, far):
    steps = 4
    shapes = dict(rc=(rows, LANES), s0=(rows, LANES), g0=(rows, LANES), rf=(far, 8, LANES))
    for level in range(1, steps + 1):
        size = rows >> (level + 1)
        shapes["r" + str(level - 1)] = shapes["s" + str(level)] = shapes["g" + str(level)] = (2, size, LANES)
    return shapes


def all_sum(win, probe, amp, m, far, chunks, order):
    bufs = []
    for _, rows in chunks:
        bufs += [pltpu.VMEM(s, jnp.float32) for s in chunk_buffers(rows, far).values()]
    bufs += [pltpu.VMEM((6, 8, LANES), jnp.float32), pltpu.VMEM((5 + far - 1, 8, LANES), jnp.float32)]
    count = COPIES_PER_CHUNK * (len(chunks) + 2)
    modes, side = probe.shape[1:3]
    rows = (2 * modes + 1) * side
    shapes = ((rows, side), m.shape, win.shape, win.shape, (2, 2, 2, side // 2, side))
    bufs = [
        pltpu.VMEM((rows, side), jnp.float32),
        pltpu.VMEM((modes, 2, side, side), jnp.float32),
        pltpu.VMEM((side, side), jnp.float32),
    ] + bufs
    return pl.pallas_call(
        functools.partial(all_sum_kernel, chunks, far, order),
        out_shape=tuple(jax.ShapeDtypeStruct(shape, jnp.float32) for shape in shapes),
        in_specs=[pl.BlockSpec(memory_space=pltpu.VMEM)] * 6,
        out_specs=(pl.BlockSpec(memory_space=pltpu.VMEM),) * 5,
        scratch_shapes=bufs + [pltpu.SemaphoreType.DMA((count,)), pltpu.SemaphoreType.DMA((count,))],
        compiler_params=pltpu.CompilerParams(collective_id=0, has_side_effects=True, vmem_limit_bytes=30 * MIB),
        name="all_sum",
    )(win, probe, amp, dft_tables(side), order_table(side), m)


def dft_tables(side):
    half = side // 2
    n, q = np.arange(half)[None, :], np.arange(half)[:, None]
    tables = []
    for odd in range(2):
        phase = 2.0 * np.pi * ((n * (2 * q + odd)) % side) / side
        cosine, sine = np.cos(phase) / math.sqrt(side), np.sin(phase) / math.sqrt(side)
        table = np.block([[cosine, sine], [-sine, cosine]])
        tables += [table, table.T]
    tables = np.stack(tables).astype(np.float32)
    high = tables.astype(jnp.bfloat16)
    low = (tables - high.astype(np.float32)).astype(jnp.bfloat16)
    return np.stack([high, low], axis=1)


def order_table(side):
    table = np.zeros((side, side), np.float32)
    at = np.arange(side)
    table[at, np.where(at < side // 2, 2 * at, 2 * at + 1 - side)] = 1.0
    return table.astype(jnp.bfloat16)


def halves(value):
    high = value.astype(jnp.bfloat16)
    return high, (value - high.astype(jnp.float32)).astype(jnp.bfloat16)


def dot(a, b):
    return jnp.dot(a, b, preferred_element_type=jnp.float32)


def from_left(tab_ref, which, value):
    high, low = halves(value)
    return dot(tab_ref[which, 0], high) + dot(tab_ref[which, 0], low) + dot(tab_ref[which, 1], high)


def from_right(tab_ref, which, value):
    high, low = halves(value)
    return dot(high, tab_ref[which, 0]) + dot(low, tab_ref[which, 0]) + dot(high, tab_ref[which, 1])


def to_far_field(tab_ref, re, im):
    h = re.shape[0] // 2
    plus = jnp.concatenate([re[:h] + re[h:], im[:h] + im[h:]], axis=0)
    minus = jnp.concatenate([re[:h] - re[h:], im[:h] - im[h:]], axis=0)
    even, odd = from_left(tab_ref, 0, plus), from_left(tab_ref, 2, minus)
    re = jnp.concatenate([even[:h], odd[:h]], axis=0)
    im = jnp.concatenate([even[h:], odd[h:]], axis=0)
    plus = jnp.concatenate([re[:, :h] + re[:, h:], im[:, :h] + im[:, h:]], axis=1)
    minus = jnp.concatenate([re[:, :h] - re[:, h:], im[:, :h] - im[:, h:]], axis=1)
    even, odd = from_right(tab_ref, 1, plus), from_right(tab_ref, 3, minus)
    re = jnp.concatenate([even[:, :h], odd[:, :h]], axis=1)
    im = jnp.concatenate([even[:, h:], odd[:, h:]], axis=1)
    return re, im


def from_far_field(tab_ref, re, im):
    h = re.shape[0] // 2
    even = from_right(tab_ref, 0, jnp.concatenate([re[:, :h], im[:, :h]], axis=1))
    odd = from_right(tab_ref, 2, jnp.concatenate([re[:, h:], im[:, h:]], axis=1))
    plus, minus = even + odd, even - odd
    re = jnp.concatenate([plus[:, :h], minus[:, :h]], axis=1)
    im = jnp.concatenate([plus[:, h:], minus[:, h:]], axis=1)
    even = from_left(tab_ref, 1, jnp.concatenate([re[:h], im[:h]], axis=0))
    odd = from_left(tab_ref, 3, jnp.concatenate([re[h:], im[h:]], axis=0))
    plus, minus = even + odd, even - odd
    re = jnp.concatenate([plus[:h], minus[:h]], axis=0)
    im = jnp.concatenate([plus[h:], minus[h:]], axis=0)
    return re, im


def reorder(order_ref, value):
    def three(v):
        high, rest = v.astype(jnp.bfloat16), None
        rest = v - high.astype(jnp.float32)
        middle = rest.astype(jnp.bfloat16)
        return high, middle, (rest - middle.astype(jnp.float32)).astype(jnp.bfloat16)

    table = order_ref[...]
    high, middle, low = three(value)
    value = dot(table, high) + dot(table, middle) + dot(table, low)
    across = lambda v: lax.dot_general(
        v, table, (((1,), (1,)), ((), ())), preferred_element_type=jnp.float32
    )
    high, middle, low = three(value)
    return across(high) + across(middle) + across(low)


def from_row(ref, row, rows, cols):
    off = lax.rem(row, 8)
    value = ref[pl.ds(pl.multiple_of(row - off, 8), rows + 8), cols]
    return pltpu.roll(value, lax.rem(rows + 8 - off, rows + 8), 0)[:rows]


def add_window(acc_ref, source_ref, row, col, scale=None):
    rows = acc_ref.shape[0]
    side = source_ref.shape[1]
    value = from_row(source_ref, row, rows, slice(None))
    if scale is not None:
        value = jnp.where(scale > 0, value, 0.0)
    value = jnp.concatenate([value, jnp.zeros((rows, LANES), jnp.float32)], axis=1)
    value = pltpu.roll(value, lax.rem(col, LANES), 1)
    at = pl.ds(pl.multiple_of(lax.div(col, LANES) * LANES, LANES), side + LANES)
    acc_ref[:, at] = acc_ref[:, at] + value


def sources(cent_ref, tile_cols, margin):
    c = cent_ref[6, 0]
    for where in range(3):
        for side_col in range(2):
            k = where * 2 + side_col
            row = margin - cent_ref[k, 0]
            col = (side_col - c) * tile_cols + cent_ref[k, 1] - margin + tile_cols + margin
            there = jnp.int32(1)
            if where == 0:
                there = cent_ref[7, 0]
            if where == 2:
                there = cent_ref[7, 1]
            yield where, side_col, row, col, there


def forward_waves(win, probe_ref, amp_ref, tab_ref, order_ref, far, amp):
    amp[...] = jnp.zeros_like(amp)

    def forward(m, carry):
        pr, pi = probe_ref[0, m].astype(jnp.float32), probe_ref[1, m].astype(jnp.float32)
        re, im = to_far_field(tab_ref, pr * win[0] - pi * win[1], pr * win[1] + pi * win[0])
        far[m, 0], far[m, 1] = re, im
        amp[...] += re * re + im * im
        return carry

    lax.fori_loop(0, probe_ref.shape[1], forward, 0)
    amp[...] = reorder(order_ref, amp_ref[0]) / (jnp.sqrt(amp[...]) + 0.5)


def backward_waves(first, count, win, probe_ref, tab_ref, far, amp, upd_ref, sum_ref):
    side = probe_ref.shape[2]

    def backward(m, carry):
        factor = amp[...]
        re, im = from_far_field(tab_ref, far[m, 0] * factor, far[m, 1] * factor)
        pr, pi = probe_ref[0, m].astype(jnp.float32), probe_ref[1, m].astype(jnp.float32)
        wr, wi = win[0], win[1]
        re = re - (pr * wr - pi * wi)
        im = im - (pr * wi + pi * wr)
        upd_ref[0] += pr * re + pi * im
        upd_ref[1] += pr * im - pi * re
        at_re, at_im = pl.multiple_of(2 * m * side, 8), pl.multiple_of((2 * m + 1) * side, 8)
        sum_ref[pl.ds(at_re, side), :] = wr * re + wi * im
        sum_ref[pl.ds(at_im, side), :] = wr * im - wi * re
        return carry

    lax.fori_loop(first, first + count, backward, 0)


def window_kernel(cent_ref, ext_ref, probe_ref, win_ref, illum_ref, top_ref, acc, shifted):
    modes, side = probe_ref.shape[1], probe_ref.shape[2]
    margin = side // 2
    tile_rows, tile_cols = illum_ref.shape
    c = cent_ref[6, 0]
    own_row, own_col = cent_ref[2 + c, 0], cent_ref[2 + c, 1]
    shift = lax.rem(own_col, LANES)
    at = pl.ds(pl.multiple_of(own_col - shift, LANES), side + LANES)
    for p in range(2):
        value = from_row(ext_ref.at[p], own_row, side, at)
        value = pltpu.roll(value, lax.rem(side + LANES - shift, side + LANES), 1)
        win_ref[p] = value[:, :side]
    spot = jnp.zeros((side, side), jnp.float32)
    for m in range(modes):
        pr, pi = probe_ref[0, m].astype(jnp.float32), probe_ref[1, m].astype(jnp.float32)
        spot = spot + (pr * pr + pi * pi)
    shifted[pl.ds(0, side), :] = spot
    zeros = jnp.zeros((margin, side), jnp.float32)
    spot_top, spot_bottom = shifted[pl.ds(0, margin), :], shifted[pl.ds(margin, margin), :]
    acc[...] = jnp.zeros_like(acc)
    laid = {0: (spot_bottom, zeros), 1: (spot_top, spot_bottom), 2: (zeros, spot_top)}
    for where, side_col, row, col, there in sources(cent_ref, tile_cols, margin):
        if side_col == 0:
            shifted[pl.ds(0, margin), :], shifted[pl.ds(margin, margin), :] = laid[where]
        add_window(acc, shifted, row, col, there)
    total = acc[:, pl.ds(tile_cols + margin, tile_cols)]
    illum_ref[...] = total
    top_ref[...] = jnp.full(top_ref.shape, jnp.max(total))


def place_kernel(
    cent_ref, obj_ref, probe_ref, upd_ref, pair_ref, part_ref, illum_ref, top_ref, sum_ref,
    new_obj_ref, new_probe_ref, acc, shifted,
):
    modes, side = probe_ref.shape[1], probe_ref.shape[2]
    margin = side // 2
    tile_cols = illum_ref.shape[1]
    c = cent_ref[6, 0]
    below = illum_ref[...] + 0.1 * jnp.max(top_ref[...])
    for p in range(2):
        acc[...] = jnp.zeros_like(acc)
        for where, side_col, row, col, there in sources(cent_ref, tile_cols, margin):
            if where == 1:
                shifted[pl.ds(0, side), :] = jnp.where(c == side_col, upd_ref[p], pair_ref[p])
            else:
                part = part_ref[where // 2, side_col, p]
                first = where // 2 * margin
                shifted[pl.ds(first, margin), :] = part
                shifted[pl.ds(margin - first, margin), :] = jnp.zeros((margin, side), jnp.float32)
            add_window(acc, shifted, row, col, there)
        new_obj_ref[p] = obj_ref[p] + acc[:, pl.ds(tile_cols + margin, tile_cols)] / below
    weight = sum_ref[pl.ds(2 * modes * side, side), :]
    over = weight + 0.1 * jnp.max(weight)

    def finish(m, carry):
        for p in range(2):
            at = pl.ds(pl.multiple_of((2 * m + p) * side, 8), side)
            new_probe_ref[p, m] = probe_ref[p, m].astype(jnp.float32) + sum_ref[at, :] / over
        return carry

    lax.fori_loop(0, modes, finish, 0)


def row_neighbours(x, z, near, deep):
    up = {"row_0": lax.rem(z + deep - (x == 0).astype(jnp.int32), deep), "row_1": lax.rem(x + near - 1, near)}
    down = {"row_0": lax.rem(z + (x == near - 1).astype(jnp.int32), deep), "row_1": lax.rem(x + 1, near)}
    return up, down


def halo_kernel(deep, near, obj_ref, cent_ref, ext_ref, cents_ref, send_sems, recv_sems):
    rows, cols = obj_ref.shape[1], obj_ref.shape[2]
    c, x, z = lax.axis_index("col"), lax.axis_index("row_1"), lax.axis_index("row_0")
    other = {"col": 1 - c}
    up, down = row_neighbours(x, z, near, deep)
    up_other, down_other = dict(up, **other), dict(down, **other)
    barrier = pltpu.get_barrier_semaphore()
    for peer in (other, up, down, up_other, down_other):
        pl.semaphore_signal(barrier, inc=1, device_id=peer, device_id_type=MESHID)
    pl.semaphore_wait(barrier, 5)
    tile = pl.ds(LANES, cols)
    first, last = Exchange(send_sems, recv_sems, 0), Exchange(send_sems, recv_sems, 8)
    edge = pl.ds(pl.multiple_of((1 - c) * (cols - LANES), LANES), LANES)
    held_edge = pl.ds(pl.multiple_of(LANES + (1 - c) * (cols - LANES), LANES), LANES)
    rim = pl.ds(pl.multiple_of(c * (cols + LANES), LANES), LANES)
    first.send(obj_ref, ext_ref.at[:, pl.ds(2 * rows, rows), tile], up)
    first.send(obj_ref, ext_ref.at[:, pl.ds(0, rows), tile], down)
    first.send(obj_ref.at[:, :, edge], ext_ref.at[:, pl.ds(rows, rows), rim], other)
    first.send(cent_ref, cents_ref.at[4 + c], up)
    first.send(cent_ref, cents_ref.at[4 + c], up_other)
    first.send(cent_ref, cents_ref.at[c], down)
    first.send(cent_ref, cents_ref.at[c], down_other)
    first.send(cent_ref, cents_ref.at[2 + c], other)
    cents_ref[2 + c] = cent_ref[...]
    ext_ref[:, pl.ds(rows, rows), tile] = obj_ref[...]
    ext_ref[:, :, rim] = jnp.zeros((2, 3 * rows, LANES), jnp.float32)
    for copy in first.copies[2:]:
        copy.wait()
    for i, start in ((0, 2 * rows), (1, 0)):
        first.copies[i].wait()
        here = pl.ds(start, rows)
        last.send(ext_ref.at[:, here, held_edge], ext_ref.at[:, here, rim], other)
    for copy in last.copies:
        copy.wait()

    @pl.when((x == 0) & (z == 0))
    def _():
        ext_ref[:, pl.ds(0, rows), :] = jnp.zeros((2, rows, cols + 2 * LANES), jnp.float32)

    @pl.when((x == near - 1) & (z == deep - 1))
    def _():
        ext_ref[:, pl.ds(2 * rows, rows), :] = jnp.zeros((2, rows, cols + 2 * LANES), jnp.float32)

def in_vmem(count):
    return [pl.BlockSpec(memory_space=pltpu.VMEM)] * count


def float_shapes(*shapes):
    return tuple(jax.ShapeDtypeStruct(shape, jnp.float32) for shape in shapes)


def local(obj_field, probe_modes, centers, amplitudes):
    _, tile_rows, tile_cols = obj_field.shape
    mode_count, side = probe_modes.shape[1:3]
    deep, near = lax.axis_size("row_0"), lax.axis_size("row_1")
    c, x, z = lax.axis_index("col"), lax.axis_index("row_1"), lax.axis_index("row_0")
    anchor = jnp.stack([(z * near + x) * tile_rows, c * tile_cols])
    cent = jnp.pad(centers - anchor, ((0, 7), (0, LANES - 2)))
    ext, cents = pl.pallas_call(
        functools.partial(halo_kernel, deep, near),
        out_shape=(
            jax.ShapeDtypeStruct((2, 3 * tile_rows, tile_cols + 2 * LANES), jnp.float32),
            jax.ShapeDtypeStruct((6, 8, LANES), jnp.int32),
        ),
        in_specs=in_vmem(2),
        out_specs=tuple(in_vmem(2)),
        scratch_shapes=[pltpu.SemaphoreType.DMA((16,)), pltpu.SemaphoreType.DMA((16,))],
        compiler_params=pltpu.CompilerParams(collective_id=1, has_side_effects=True, vmem_limit_bytes=6 * MIB),
        name="halo",
    )(obj_field, cent)
    row = z * near + x
    place = jnp.stack([c, c, (row > 0).astype(jnp.int32), (row < deep * near - 1).astype(jnp.int32)])
    cents = jnp.concatenate([cents[:, 0, :2], place.reshape(2, 2)], axis=0)
    planes = 2 * mode_count
    margin = side // 2
    wide = 3 * tile_cols + 2 * LANES
    win, illumination, top = pl.pallas_call(
        window_kernel,
        out_shape=float_shapes((2, side, side), (tile_rows, tile_cols), (8, LANES)),
        in_specs=[pl.BlockSpec(memory_space=pltpu.SMEM)] + in_vmem(2),
        out_specs=tuple(in_vmem(3)),
        scratch_shapes=[pltpu.VMEM((tile_rows, wide), jnp.float32), pltpu.VMEM((side + 8, side), jnp.float32)],
        compiler_params=pltpu.CompilerParams(vmem_limit_bytes=8 * MIB),
        name="window",
    )(cents, ext, probe_modes)
    share = 4 * side
    chunks = ((planes * side, side),) + tuple(
        (start, share) for start in range(0, planes * side, share)
    )
    sums, top, upd, pair, part = all_sum(win, probe_modes, amplitudes, top, deep // NEAR, chunks, ORDER)
    return pl.pallas_call(
        place_kernel,
        out_shape=float_shapes(obj_field.shape, probe_modes.shape),
        in_specs=[pl.BlockSpec(memory_space=pltpu.SMEM)] + in_vmem(8),
        out_specs=tuple(in_vmem(2)),
        scratch_shapes=[pltpu.VMEM((tile_rows, wide), jnp.float32), pltpu.VMEM((side + 8, side), jnp.float32)],
        compiler_params=pltpu.CompilerParams(vmem_limit_bytes=16 * MIB),
        name="place",
    )(cents, obj_field, probe_modes, upd, pair, part, illumination, top, sums)


def solution(mesh):
    split = Mesh(
        mesh.devices.reshape(mesh.shape["angle"], mesh.shape["row"] // 4, 4, mesh.shape["col"]),
        ("angle", "row_0", "row_1", "col"),
    )
    return jax.shard_map(
        local,
        mesh=split,
        in_specs=(
            P(None, ANGLE_ROW, "col"),
            P(),
            P(ANGLE_ROW_COL, None),
            P(ANGLE_ROW_COL, None, None),
        ),
        out_specs=(P(None, ANGLE_ROW, "col"), P(None, "angle", None, None)),
        check_vma=False,
    )
```

```python
import functools
import math

import jax
import jax.numpy as jnp
import numpy as np
from jax import lax
from jax.experimental import pallas as pl
from jax.experimental.pallas import tpu as pltpu
from jax.sharding import Mesh
from jax.sharding import PartitionSpec as P

ROW = ("row_0", "row_1")
ANGLE_ROW = ("angle", "row_0", "row_1")
ANGLE_ROW_COL = ("angle", "row_0", "row_1", "col")
MIB = 1024 * 1024
BEFORE_BARRIER = (0, 1)
ORDER = (
    (0, 0), (-1, 0), (1, 0), (2, 0), (-3, 2), (3, 0), (0, 1), (-1, 1), (1, 1), (2, 1),
    (3, 1), (0, 2), (-1, 2), (1, 2), (2, 2), (3, 2), (0, 3), (-1, 3), (1, 3), (2, 3),
    (3, 3), (0, 4), (-1, 4), (1, 4), (2, 4), (3, 4), (-2, 0), (0, 5), (-1, 5), (1, 5),
    (2, 5), (3, 5), (0, 6), (1, 6), (2, 6), (3, 6), (-2, 1), (0, 7), (1, 7), (2, 7),
    (3, 7), (0, 8), (1, 8), (2, 8), (3, 8), (0, 9), (1, 9), (2, 9), (3, 9), (-2, 2),
)

MESHID = pl.DeviceIdType.MESH
LANES = 128
NEAR = 4


class Exchange:
    def __init__(self, send_sems, recv_sems, first):
        self.send_sems, self.recv_sems, self.next = send_sems, recv_sems, first
        self.copies = []

    def send(self, src, dst, peer):
        copy = pltpu.make_async_remote_copy(
            src_ref=src,
            dst_ref=dst,
            send_sem=self.send_sems.at[self.next],
            recv_sem=self.recv_sems.at[self.next],
            device_id=peer,
            device_id_type=MESHID,
        )
        copy.start()
        self.next += 1
        self.copies.append(copy)


def rows_at(ref, start, size):
    return ref.at[pl.ds(pl.multiple_of(start, 8), size), :]


def far_order(count):
    return sorted(range(1, count), key=lambda d: -min(d, count - d))


COPIES_PER_CHUNK = 64


def all_sum_kernel(
    chunks, far, order, win_ref, probe_ref, amp_ref, tab_ref, order_ref, m_ref,
    o_ref, om_ref, upd_ref, pair_ref, part_ref, x_ref, waves, factor, *scratch,
):
    scratch = list(scratch)
    modes, side = probe_ref.shape[1], probe_ref.shape[2]
    send_sems, recv_sems = scratch[-2:]
    c, x, z = lax.axis_index("col"), lax.axis_index("row_1"), lax.axis_index("row_0")
    near_at, far_at = lax.rem(z, NEAR), lax.div(z, NEAR)
    partner = {"col": 1 - c}
    x_one = {"row_1": x + 1 - 2 * lax.rem(x, 2)}
    x_two = {"row_1": 3 - x}
    near_peers = {d: {"row_0": far_at * NEAR + lax.rem(near_at + d, NEAR)} for d in range(1, NEAR)}
    far_peers = {d: {"row_0": lax.rem(far_at + d, far) * NEAR + near_at} for d in range(1, far)}
    near_order, far_list = far_order(NEAR), far_order(far)
    barrier = pltpu.get_barrier_semaphore()
    up, down = row_neighbours(x, z, 4, far * NEAR)
    peers = [partner, x_one, x_two, up, down, *near_peers.values(), *far_peers.values()]
    for peer in peers:
        pl.semaphore_signal(barrier, inc=1, device_id=peer, device_id_type=MESHID)
    x_ref[pl.ds(2 * modes * side, side), :] = win_ref[0] * win_ref[0] + win_ref[1] * win_ref[1]
    upd_ref[...] = jnp.zeros_like(upd_ref)
    forward_waves(win_ref, probe_ref, amp_ref, tab_ref, order_ref, waves, factor)

    def modes_back(group):
        per = chunks[1][1] // (2 * side)
        backward_waves(group * per, per, win_ref, probe_ref, tab_ref, waves, factor, upd_ref, x_ref)

    for group in BEFORE_BARRIER:
        modes_back(group)
    pl.semaphore_wait(barrier, len(peers))

    mine, theirs = (
        pl.ds(pl.multiple_of(c * LANES, LANES), LANES),
        pl.ds(pl.multiple_of((1 - c) * LANES, LANES), LANES),
    )
    bit_a = lax.rem(lax.div(x + 1, 2), 2)
    bit_b = lax.div(x, 2)
    keep_one, peer_one = (bit_a, bit_b), (x_one, x_two)
    keep_two, peer_two = (bit_b, bit_a), (x_two, x_one)

    class Chunk:
        def __init__(self, index, start, rows, bufs):
            self.start, self.rows, self.bufs = start, rows, bufs
            self.next = index * COPIES_PER_CHUNK
            self.spread = rows // 128 >= 8
            self.pending = None

        def exchange(self):
            self.pending = Exchange(send_sems, recv_sems, self.next)
            return self.pending

        def arrive(self):
            for copy in self.pending.copies:
                copy.wait()
            self.next = self.pending.next

        def step(self, s):
            R, b = self.rows, self.bufs
            if s > 0:
                self.arrive()
            if s == 0:
                e = self.exchange()
                e.send(x_ref.at[pl.ds(self.start, R), theirs], b["rc"], partner)
            elif s == 1:
                b["s0"][...] = x_ref[pl.ds(self.start, R), mine] + b["rc"][...]
                e = self.exchange()
                for h in range(2):
                    src = rows_at(b["s0"], h * (R // 2) + (1 - keep_one[h]) * (R // 4), R // 4)
                    e.send(src, b["r1"].at[h], peer_one[h])
            elif s == 2:
                for h in range(2):
                    kept = pl.ds(pl.multiple_of(h * (R // 2) + keep_one[h] * (R // 4), 8), R // 4)
                    b["s1"][h] = b["s0"][kept, :] + b["r1"][h]
                e = self.exchange()
                for h in range(2):
                    src = rows_at(b["s1"].at[h], (1 - keep_two[h]) * (R // 8), R // 8)
                    e.send(src, b["r2"].at[h], peer_two[h])
            elif s == 3:
                for h in range(2):
                    kept = pl.ds(pl.multiple_of(keep_two[h] * (R // 8), 8), R // 8)
                    b["s2"][pl.ds(h * (R // 8), R // 8), :] = b["s1"][h, kept, :] + b["r2"][h]
                e = self.exchange()
                for d in near_order:
                    src = rows_at(b["s2"], lax.rem(near_at + d, NEAR) * (R // 16), R // 16)
                    e.send(src, b["r3"].at[d - 1], near_peers[d])
            elif s == 4:
                kept = pl.ds(pl.multiple_of(near_at * (R // 16), 8), R // 16)
                total = b["s2"][kept, :]
                for d in range(1, NEAR):
                    total = total + b["r3"][d - 1]
                b["s3"][...] = total
                e = self.exchange()
                for d in far_list:
                    if self.spread:
                        src = rows_at(b["s3"], lax.rem(far_at + d, far) * (R // 128), R // 128)
                    else:
                        src = b["s3"]
                    e.send(src, b["r4"].at[d - 1], far_peers[d])
            elif s == 5:
                if self.spread:
                    at = pl.ds(pl.multiple_of(far_at * (R // 128), 8), R // 128)
                    total = b["s3"][at, :]
                    for d in range(1, far):
                        total = total + b["r4"][d - 1]
                    b["g3"][at, :] = total
                    e = self.exchange()
                    block = rows_at(b["g3"], far_at * (R // 128), R // 128)
                    for d in far_list:
                        e.send(block, block, far_peers[d])
                else:
                    b["r4"][far - 1] = b["s3"][...]
                    total = jnp.zeros((R // 16, LANES), jnp.float32)
                    for owner in range(far):
                        total = total + b["r4"][lax.rem(far_at - owner + far - 1, far)]
                    b["g3"][...] = total
                    self.exchange()
            elif s == 6:
                at = pl.ds(pl.multiple_of(near_at * (R // 16), 8), R // 16)
                e = self.exchange()
                dst = rows_at(b["g2"], near_at * (R // 16), R // 16)
                for d in near_order:
                    e.send(b["g3"], dst, near_peers[d])
                b["g2"][at, :] = b["g3"][...]
            elif s == 7:
                e = self.exchange()
                for h in range(2):
                    src = rows_at(b["g2"], h * (R // 8), R // 8)
                    dst = rows_at(b["g1"].at[h], keep_two[h] * (R // 8), R // 8)
                    e.send(src, dst, peer_two[h])
                for h in range(2):
                    at = pl.ds(pl.multiple_of(keep_two[h] * (R // 8), 8), R // 8)
                    b["g1"][h, at, :] = b["g2"][pl.ds(h * (R // 8), R // 8), :]
            elif s == 8:
                e = self.exchange()
                for h in range(2):
                    dst = rows_at(b["g0"], h * (R // 2) + keep_one[h] * (R // 4), R // 4)
                    e.send(b["g1"].at[h], dst, peer_one[h])
                for h in range(2):
                    at = pl.ds(pl.multiple_of(h * (R // 2) + keep_one[h] * (R // 4), 8), R // 4)
                    b["g0"][at, :] = b["g1"][h]
            elif s == 9:
                e = self.exchange()
                e.send(b["g0"], o_ref.at[pl.ds(self.start, R), mine], partner)
                o_ref[pl.ds(self.start, R), mine] = b["g0"][...]

    class Peak:
        def __init__(self, index, bufs):
            self.next, self.bufs = index * COPIES_PER_CHUNK, bufs
            self.stages = [[partner], [x_one], [x_two], list(near_peers.values()), list(far_peers.values())]
            self.slot = 0
            self.copies = []

        def step(self, s):
            held, came = self.bufs["held"], self.bufs["came"]
            if s > 0:
                top = m_ref[...] if s == 1 else held[s - 1]
                for i, copy in enumerate(self.copies):
                    copy.wait()
                    top = jnp.maximum(top, came[self.slot - len(self.copies) + i])
                if s == 5:
                    om_ref[...] = top
                    return
                held[s] = top
            e = Exchange(send_sems, recv_sems, self.next)
            for peer in self.stages[s]:
                e.send(m_ref if s == 0 else held.at[s], came.at[self.slot], peer)
                self.slot += 1
            self.next, self.copies = e.next, e.copies

    class Fold:
        def __init__(self, index):
            self.index = index

        def step(self, s):
            half = upd_ref.shape[1] // 2
            if s == 0:
                self.first = Exchange(send_sems, recv_sems, self.index * COPIES_PER_CHUNK)
                self.first.send(upd_ref.at[:, pl.ds(half, half), :], part_ref.at[0, c], down)
                self.first.send(upd_ref.at[:, pl.ds(0, half), :], part_ref.at[1, c], up)
                self.first.send(upd_ref, pair_ref, partner)
            elif s == 1:
                self.last = Exchange(send_sems, recv_sems, self.index * COPIES_PER_CHUNK + 8)
                for i in range(2):
                    self.first.copies[i].wait()
                    self.last.send(part_ref.at[i, c], part_ref.at[i, c], partner)
                self.first.copies[2].wait()
            else:
                for copy in self.last.copies:
                    copy.wait()

    fold = Fold(len(chunks) + 1)
    objects = []
    at = 0
    for i, (start, rows) in enumerate(chunks):
        names = chunk_buffers(rows, far)
        bufs = dict(zip(names, scratch[at : at + len(names)]))
        at += len(names)
        objects.append(Chunk(i, start, rows, bufs))
    peak = Peak(len(chunks), dict(held=scratch[at], came=scratch[at + 1]))
    for which, s in order:
        if which == -1:
            peak.step(s)
        elif which == -2:
            fold.step(s)
        elif which == -3:
            modes_back(s)
        else:
            objects[which].step(s)
    for o in objects:
        o.arrive()


def chunk_buffers(rows, far):
    R = rows
    last = R // 128 if R // 128 >= 8 else R // 16
    return dict(
        rc=(R, LANES), s0=(R, LANES), r1=(2, R // 4, LANES), s1=(2, R // 4, LANES), r2=(2, R // 8, LANES),
        s2=(R // 4, LANES), r3=(NEAR - 1, R // 16, LANES), s3=(R // 16, LANES), r4=(far, last, LANES),
        g3=(R // 16, LANES), g2=(R // 4, LANES), g1=(2, R // 4, LANES), g0=(R, LANES),
    )


def all_sum(win, probe, amp, m, far, chunks, order):
    bufs = []
    for _, rows in chunks:
        bufs += [pltpu.VMEM(s, jnp.float32) for s in chunk_buffers(rows, far).values()]
    bufs += [pltpu.VMEM((6, 8, LANES), jnp.float32), pltpu.VMEM((3 + NEAR - 1 + far - 1, 8, LANES), jnp.float32)]
    count = COPIES_PER_CHUNK * (len(chunks) + 2)
    modes, side = probe.shape[1:3]
    rows = (2 * modes + 1) * side
    shapes = ((rows, side), m.shape, win.shape, win.shape, (2, 2, 2, side // 2, side))
    bufs = [
        pltpu.VMEM((rows, side), jnp.float32),
        pltpu.VMEM((modes, 2, side, side), jnp.float32),
        pltpu.VMEM((side, side), jnp.float32),
    ] + bufs
    return pl.pallas_call(
        functools.partial(all_sum_kernel, chunks, far, order),
        out_shape=tuple(jax.ShapeDtypeStruct(shape, jnp.float32) for shape in shapes),
        in_specs=[pl.BlockSpec(memory_space=pltpu.VMEM)] * 6,
        out_specs=(pl.BlockSpec(memory_space=pltpu.VMEM),) * 5,
        scratch_shapes=bufs + [pltpu.SemaphoreType.DMA((count,)), pltpu.SemaphoreType.DMA((count,))],
        compiler_params=pltpu.CompilerParams(collective_id=0, has_side_effects=True, vmem_limit_bytes=30 * MIB),
        name="all_sum",
    )(win, probe, amp, dft_tables(side), order_table(side), m)


def dft_tables(side):
    half = side // 2
    n, q = np.arange(half)[None, :], np.arange(half)[:, None]
    tables = []
    for odd in range(2):
        phase = 2.0 * np.pi * ((n * (2 * q + odd)) % side) / side
        cosine, sine = np.cos(phase) / math.sqrt(side), np.sin(phase) / math.sqrt(side)
        table = np.block([[cosine, sine], [-sine, cosine]])
        tables += [table, table.T]
    tables = np.stack(tables).astype(np.float32)
    high = tables.astype(jnp.bfloat16)
    low = (tables - high.astype(np.float32)).astype(jnp.bfloat16)
    return np.stack([high, low], axis=1)


def order_table(side):
    table = np.zeros((side, side), np.float32)
    at = np.arange(side)
    table[at, np.where(at < side // 2, 2 * at, 2 * at + 1 - side)] = 1.0
    return table.astype(jnp.bfloat16)


def halves(value):
    high = value.astype(jnp.bfloat16)
    return high, (value - high.astype(jnp.float32)).astype(jnp.bfloat16)


def dot(a, b):
    return jnp.dot(a, b, preferred_element_type=jnp.float32)


def from_left(tab_ref, which, value):
    high, low = halves(value)
    return dot(tab_ref[which, 0], high) + dot(tab_ref[which, 0], low) + dot(tab_ref[which, 1], high)


def from_right(tab_ref, which, value):
    high, low = halves(value)
    return dot(high, tab_ref[which, 0]) + dot(low, tab_ref[which, 0]) + dot(high, tab_ref[which, 1])


def to_far_field(tab_ref, re, im):
    h = re.shape[0] // 2
    plus = jnp.concatenate([re[:h] + re[h:], im[:h] + im[h:]], axis=0)
    minus = jnp.concatenate([re[:h] - re[h:], im[:h] - im[h:]], axis=0)
    even, odd = from_left(tab_ref, 0, plus), from_left(tab_ref, 2, minus)
    re = jnp.concatenate([even[:h], odd[:h]], axis=0)
    im = jnp.concatenate([even[h:], odd[h:]], axis=0)
    plus = jnp.concatenate([re[:, :h] + re[:, h:], im[:, :h] + im[:, h:]], axis=1)
    minus = jnp.concatenate([re[:, :h] - re[:, h:], im[:, :h] - im[:, h:]], axis=1)
    even, odd = from_right(tab_ref, 1, plus), from_right(tab_ref, 3, minus)
    re = jnp.concatenate([even[:, :h], odd[:, :h]], axis=1)
    im = jnp.concatenate([even[:, h:], odd[:, h:]], axis=1)
    return re, im


def from_far_field(tab_ref, re, im):
    h = re.shape[0] // 2
    even = from_right(tab_ref, 0, jnp.concatenate([re[:, :h], im[:, :h]], axis=1))
    odd = from_right(tab_ref, 2, jnp.concatenate([re[:, h:], im[:, h:]], axis=1))
    plus, minus = even + odd, even - odd
    re = jnp.concatenate([plus[:, :h], minus[:, :h]], axis=1)
    im = jnp.concatenate([plus[:, h:], minus[:, h:]], axis=1)
    even = from_left(tab_ref, 1, jnp.concatenate([re[:h], im[:h]], axis=0))
    odd = from_left(tab_ref, 3, jnp.concatenate([re[h:], im[h:]], axis=0))
    plus, minus = even + odd, even - odd
    re = jnp.concatenate([plus[:h], minus[:h]], axis=0)
    im = jnp.concatenate([plus[h:], minus[h:]], axis=0)
    return re, im


def reorder(order_ref, value):
    def three(v):
        high, rest = v.astype(jnp.bfloat16), None
        rest = v - high.astype(jnp.float32)
        middle = rest.astype(jnp.bfloat16)
        return high, middle, (rest - middle.astype(jnp.float32)).astype(jnp.bfloat16)

    table = order_ref[...]
    high, middle, low = three(value)
    value = dot(table, high) + dot(table, middle) + dot(table, low)
    across = lambda v: lax.dot_general(
        v, table, (((1,), (1,)), ((), ())), preferred_element_type=jnp.float32
    )
    high, middle, low = three(value)
    return across(high) + across(middle) + across(low)


def from_row(ref, row, rows, cols):
    off = lax.rem(row, 8)
    value = ref[pl.ds(pl.multiple_of(row - off, 8), rows + 8), cols]
    return pltpu.roll(value, lax.rem(rows + 8 - off, rows + 8), 0)[:rows]


def add_window(acc_ref, source_ref, row, col, scale=None):
    rows = acc_ref.shape[0]
    side = source_ref.shape[1]
    value = from_row(source_ref, row, rows, slice(None))
    if scale is not None:
        value = jnp.where(scale > 0, value, 0.0)
    value = jnp.concatenate([value, jnp.zeros((rows, LANES), jnp.float32)], axis=1)
    value = pltpu.roll(value, lax.rem(col, LANES), 1)
    at = pl.ds(pl.multiple_of(lax.div(col, LANES) * LANES, LANES), side + LANES)
    acc_ref[:, at] = acc_ref[:, at] + value


def sources(cent_ref, tile_cols, margin):
    c = cent_ref[6, 0]
    for where in range(3):
        for side_col in range(2):
            k = where * 2 + side_col
            row = margin - cent_ref[k, 0]
            col = (side_col - c) * tile_cols + cent_ref[k, 1] - margin + tile_cols + margin
            there = jnp.int32(1)
            if where == 0:
                there = cent_ref[7, 0]
            if where == 2:
                there = cent_ref[7, 1]
            yield where, side_col, row, col, there


def forward_waves(win, probe_ref, amp_ref, tab_ref, order_ref, far, amp):
    amp[...] = jnp.zeros_like(amp)

    def forward(m, carry):
        pr, pi = probe_ref[0, m].astype(jnp.float32), probe_ref[1, m].astype(jnp.float32)
        re, im = to_far_field(tab_ref, pr * win[0] - pi * win[1], pr * win[1] + pi * win[0])
        far[m, 0], far[m, 1] = re, im
        amp[...] += re * re + im * im
        return carry

    lax.fori_loop(0, probe_ref.shape[1], forward, 0)
    amp[...] = reorder(order_ref, amp_ref[0]) / (jnp.sqrt(amp[...]) + 0.5)


def backward_waves(first, count, win, probe_ref, tab_ref, far, amp, upd_ref, sum_ref):
    side = probe_ref.shape[2]

    def backward(m, carry):
        factor = amp[...]
        re, im = from_far_field(tab_ref, far[m, 0] * factor, far[m, 1] * factor)
        pr, pi = probe_ref[0, m].astype(jnp.float32), probe_ref[1, m].astype(jnp.float32)
        wr, wi = win[0], win[1]
        re = re - (pr * wr - pi * wi)
        im = im - (pr * wi + pi * wr)
        upd_ref[0] += pr * re + pi * im
        upd_ref[1] += pr * im - pi * re
        at_re, at_im = pl.multiple_of(2 * m * side, 8), pl.multiple_of((2 * m + 1) * side, 8)
        sum_ref[pl.ds(at_re, side), :] = wr * re + wi * im
        sum_ref[pl.ds(at_im, side), :] = wr * im - wi * re
        return carry

    lax.fori_loop(first, first + count, backward, 0)


def window_kernel(cent_ref, ext_ref, probe_ref, win_ref, illum_ref, top_ref, acc, shifted):
    modes, side = probe_ref.shape[1], probe_ref.shape[2]
    margin = side // 2
    tile_rows, tile_cols = illum_ref.shape
    c = cent_ref[6, 0]
    own_row, own_col = cent_ref[2 + c, 0], cent_ref[2 + c, 1]
    shift = lax.rem(own_col, LANES)
    at = pl.ds(pl.multiple_of(own_col - shift, LANES), side + LANES)
    for p in range(2):
        value = from_row(ext_ref.at[p], own_row, side, at)
        value = pltpu.roll(value, lax.rem(side + LANES - shift, side + LANES), 1)
        win_ref[p] = value[:, :side]
    spot = jnp.zeros((side, side), jnp.float32)
    for m in range(modes):
        pr, pi = probe_ref[0, m].astype(jnp.float32), probe_ref[1, m].astype(jnp.float32)
        spot = spot + (pr * pr + pi * pi)
    shifted[pl.ds(0, side), :] = spot
    zeros = jnp.zeros((margin, side), jnp.float32)
    spot_top, spot_bottom = shifted[pl.ds(0, margin), :], shifted[pl.ds(margin, margin), :]
    acc[...] = jnp.zeros_like(acc)
    laid = {0: (spot_bottom, zeros), 1: (spot_top, spot_bottom), 2: (zeros, spot_top)}
    for where, side_col, row, col, there in sources(cent_ref, tile_cols, margin):
        if side_col == 0:
            shifted[pl.ds(0, margin), :], shifted[pl.ds(margin, margin), :] = laid[where]
        add_window(acc, shifted, row, col, there)
    total = acc[:, pl.ds(tile_cols + margin, tile_cols)]
    illum_ref[...] = total
    top_ref[...] = jnp.full(top_ref.shape, jnp.max(total))


def place_kernel(
    cent_ref, obj_ref, probe_ref, upd_ref, pair_ref, part_ref, illum_ref, top_ref, sum_ref,
    new_obj_ref, new_probe_ref, acc, shifted,
):
    modes, side = probe_ref.shape[1], probe_ref.shape[2]
    margin = side // 2
    tile_cols = illum_ref.shape[1]
    c = cent_ref[6, 0]
    below = illum_ref[...] + 0.1 * jnp.max(top_ref[...])
    for p in range(2):
        acc[...] = jnp.zeros_like(acc)
        for where, side_col, row, col, there in sources(cent_ref, tile_cols, margin):
            if where == 1:
                shifted[pl.ds(0, side), :] = jnp.where(c == side_col, upd_ref[p], pair_ref[p])
            else:
                part = part_ref[where // 2, side_col, p]
                first = where // 2 * margin
                shifted[pl.ds(first, margin), :] = part
                shifted[pl.ds(margin - first, margin), :] = jnp.zeros((margin, side), jnp.float32)
            add_window(acc, shifted, row, col, there)
        new_obj_ref[p] = obj_ref[p] + acc[:, pl.ds(tile_cols + margin, tile_cols)] / below
    weight = sum_ref[pl.ds(2 * modes * side, side), :]
    over = weight + 0.1 * jnp.max(weight)

    def finish(m, carry):
        for p in range(2):
            at = pl.ds(pl.multiple_of((2 * m + p) * side, 8), side)
            new_probe_ref[p, m] = probe_ref[p, m].astype(jnp.float32) + sum_ref[at, :] / over
        return carry

    lax.fori_loop(0, modes, finish, 0)


def row_neighbours(x, z, near, deep):
    up = {"row_0": lax.rem(z + deep - (x == 0).astype(jnp.int32), deep), "row_1": lax.rem(x + near - 1, near)}
    down = {"row_0": lax.rem(z + (x == near - 1).astype(jnp.int32), deep), "row_1": lax.rem(x + 1, near)}
    return up, down


def halo_kernel(deep, near, obj_ref, cent_ref, ext_ref, cents_ref, send_sems, recv_sems):
    rows, cols = obj_ref.shape[1], obj_ref.shape[2]
    c, x, z = lax.axis_index("col"), lax.axis_index("row_1"), lax.axis_index("row_0")
    other = {"col": 1 - c}
    up, down = row_neighbours(x, z, near, deep)
    up_other, down_other = dict(up, **other), dict(down, **other)
    barrier = pltpu.get_barrier_semaphore()
    for peer in (other, up, down, up_other, down_other):
        pl.semaphore_signal(barrier, inc=1, device_id=peer, device_id_type=MESHID)
    pl.semaphore_wait(barrier, 5)
    tile = pl.ds(LANES, cols)
    first, last = Exchange(send_sems, recv_sems, 0), Exchange(send_sems, recv_sems, 8)
    edge = pl.ds(pl.multiple_of((1 - c) * (cols - LANES), LANES), LANES)
    held_edge = pl.ds(pl.multiple_of(LANES + (1 - c) * (cols - LANES), LANES), LANES)
    rim = pl.ds(pl.multiple_of(c * (cols + LANES), LANES), LANES)
    first.send(obj_ref, ext_ref.at[:, pl.ds(2 * rows, rows), tile], up)
    first.send(obj_ref, ext_ref.at[:, pl.ds(0, rows), tile], down)
    first.send(obj_ref.at[:, :, edge], ext_ref.at[:, pl.ds(rows, rows), rim], other)
    first.send(cent_ref, cents_ref.at[4 + c], up)
    first.send(cent_ref, cents_ref.at[4 + c], up_other)
    first.send(cent_ref, cents_ref.at[c], down)
    first.send(cent_ref, cents_ref.at[c], down_other)
    first.send(cent_ref, cents_ref.at[2 + c], other)
    cents_ref[2 + c] = cent_ref[...]
    ext_ref[:, pl.ds(rows, rows), tile] = obj_ref[...]
    ext_ref[:, :, rim] = jnp.zeros((2, 3 * rows, LANES), jnp.float32)
    for copy in first.copies[2:]:
        copy.wait()
    for i, start in ((0, 2 * rows), (1, 0)):
        first.copies[i].wait()
        here = pl.ds(start, rows)
        last.send(ext_ref.at[:, here, held_edge], ext_ref.at[:, here, rim], other)
    for copy in last.copies:
        copy.wait()

    @pl.when((x == 0) & (z == 0))
    def _():
        ext_ref[:, pl.ds(0, rows), :] = jnp.zeros((2, rows, cols + 2 * LANES), jnp.float32)

    @pl.when((x == near - 1) & (z == deep - 1))
    def _():
        ext_ref[:, pl.ds(2 * rows, rows), :] = jnp.zeros((2, rows, cols + 2 * LANES), jnp.float32)

def in_vmem(count):
    return [pl.BlockSpec(memory_space=pltpu.VMEM)] * count


def float_shapes(*shapes):
    return tuple(jax.ShapeDtypeStruct(shape, jnp.float32) for shape in shapes)


def local(obj_field, probe_modes, centers, amplitudes):
    _, tile_rows, tile_cols = obj_field.shape
    mode_count, side = probe_modes.shape[1:3]
    deep, near = lax.axis_size("row_0"), lax.axis_size("row_1")
    c, x, z = lax.axis_index("col"), lax.axis_index("row_1"), lax.axis_index("row_0")
    anchor = jnp.stack([(z * near + x) * tile_rows, c * tile_cols])
    cent = jnp.pad(centers - anchor, ((0, 7), (0, LANES - 2)))
    ext, cents = pl.pallas_call(
        functools.partial(halo_kernel, deep, near),
        out_shape=(
            jax.ShapeDtypeStruct((2, 3 * tile_rows, tile_cols + 2 * LANES), jnp.float32),
            jax.ShapeDtypeStruct((6, 8, LANES), jnp.int32),
        ),
        in_specs=in_vmem(2),
        out_specs=tuple(in_vmem(2)),
        scratch_shapes=[pltpu.SemaphoreType.DMA((16,)), pltpu.SemaphoreType.DMA((16,))],
        compiler_params=pltpu.CompilerParams(collective_id=1, has_side_effects=True, vmem_limit_bytes=6 * MIB),
        name="halo",
    )(obj_field, cent)
    row = z * near + x
    place = jnp.stack([c, c, (row > 0).astype(jnp.int32), (row < deep * near - 1).astype(jnp.int32)])
    cents = jnp.concatenate([cents[:, 0, :2], place.reshape(2, 2)], axis=0)
    planes = 2 * mode_count
    margin = side // 2
    wide = 3 * tile_cols + 2 * LANES
    win, illumination, top = pl.pallas_call(
        window_kernel,
        out_shape=float_shapes((2, side, side), (tile_rows, tile_cols), (8, LANES)),
        in_specs=[pl.BlockSpec(memory_space=pltpu.SMEM)] + in_vmem(2),
        out_specs=tuple(in_vmem(3)),
        scratch_shapes=[pltpu.VMEM((tile_rows, wide), jnp.float32), pltpu.VMEM((side + 8, side), jnp.float32)],
        compiler_params=pltpu.CompilerParams(vmem_limit_bytes=8 * MIB),
        name="window",
    )(cents, ext, probe_modes)
    share = 4 * side
    chunks = ((planes * side, side),) + tuple(
        (start, share) for start in range(0, planes * side, share)
    )
    sums, top, upd, pair, part = all_sum(win, probe_modes, amplitudes, top, deep // NEAR, chunks, ORDER)
    return pl.pallas_call(
        place_kernel,
        out_shape=float_shapes(obj_field.shape, probe_modes.shape),
        in_specs=[pl.BlockSpec(memory_space=pltpu.SMEM)] + in_vmem(8),
        out_specs=tuple(in_vmem(2)),
        scratch_shapes=[pltpu.VMEM((tile_rows, wide), jnp.float32), pltpu.VMEM((side + 8, side), jnp.float32)],
        compiler_params=pltpu.CompilerParams(vmem_limit_bytes=16 * MIB),
        name="place",
    )(cents, obj_field, probe_modes, upd, pair, part, illumination, top, sums)


def solution(mesh):
    split = Mesh(
        mesh.devices.reshape(mesh.shape["angle"], mesh.shape["row"] // 4, 4, mesh.shape["col"]),
        ("angle", "row_0", "row_1", "col"),
    )
    return jax.shard_map(
        local,
        mesh=split,
        in_specs=(
            P(None, ANGLE_ROW, "col"),
            P(),
            P(ANGLE_ROW_COL, None),
            P(ANGLE_ROW_COL, None, None),
        ),
        out_specs=(P(None, ANGLE_ROW, "col"), P(None, "angle", None, None)),
        check_vma=False,
    )
```
